512 devices in a mesh: band: 64 (over z, x), member: 8 (over y, core).
Axes of the slice: x: 4, y: 4, z: 16, core: 2. Of those that a mesh axis runs over, the one named last changes fastest.
Arguments:
- scaled_atmosphere_field: float32 [80, 16384], P(None, 'band'), may hold values from -6 to 6
- perturbation: bfloat16 [8, 80, 16384], P('member', None, 'band'), may hold values from -6 to 6
- target: bfloat16 [8, 80, 16384], P('member', None, 'band'), may hold values from -6 to 6
- weight_map: bfloat16 [80, 16384], P(None, 'band'), may hold values from 0.01 to 10
- enc_send: int32 [64, 64, 8], P('band'), may hold values from -1 to 255, as said below
- enc_recv: int32 [64, 64, 8], P('band'), may hold values from -1 to 255, as said below
- dec_send: int32 [64, 64, 8], P('band'), may hold values from -1 to 255, as said below
- dec_recv: int32 [64, 64, 8], P('band'), may hold values from -1 to 255, as said below
- lattice_lift_matrix: bfloat16 [80, 512], replicated, may hold values from -0.625 to 0.625
- mixing_rescale_factor: float32 [512], replicated, may hold values from 0.1 to 1.9
- expand_matrix: bfloat16 [512, 512], replicated, may hold values from -0.25 to 0.25
- contract_matrix: bfloat16 [512, 512], replicated, may hold values from -0.25 to 0.25
- readout_matrix: bfloat16 [512, 80], replicated, may hold values from -0.25 to 0.25
Outputs:
- student_outputs: float32 [8, 80, 16384], P('member', None, 'band')
- mesh_grad: bfloat16 [8, 16384, 512], P('member', 'band')
- grad_up: float32 [8, 512, 512], P('member')
- grad_down: float32 [8, 512, 512], P('member')
- grad_dec: float32 [8, 512, 80], P('member')
- grad_gain: float32 [8, 512], P('member')
The draws below stay inside these ranges and needn't reach their ends.
Inputs may be any that keep to these rules, and one draw needn't show every extreme that they name: enc_send[s, d, k] is a local grid cell of band s (0 to 255) or -1 for an empty slot; in every draw one band fills all its slots and one partition receives full blocks of 8 from every band. enc_recv[d, s, k] is a local mesh node of partition d, and -1 exactly where enc_send[s, d, k] is -1. dec_send[s, d, k] is a local mesh node of partition s or -1 for an empty slot; in every draw one partition fills all its slots and one band receives full blocks of 8 from every partition. dec_recv[d, s, k] is a local grid cell of band d, and -1 exactly where dec_send[s, d, k] is -1.
All inputs are finite; a program needn't handle non-finite values.
Results may differ from the reference program's by a relative error of at most 0.0062.
Values may be sent and summed in bfloat16 or wider, within the bound.
A program may use at most 64 MiB of HBM per device.

```python
import math
import jax
import jax.numpy as jnp
from jax import lax

CH = 80
LAT = 512
HID = 512
GRID_DEV = 256
MESH_DEV = 256
BANDS = 64
MEMBERS = 8
NGRID = 16384
NMESH = 16384
ENC_CAP = 8
DEC_CAP = 8


def draw_weight_map(key, part):
    band = (jnp.arange(NGRID, dtype=jnp.int32) // GRID_DEV).astype(jnp.float32)
    steps = float(max(BANDS - 1, 1))
    rise = jnp.exp(math.log(100.0) * (band - steps) / steps)
    base = jnp.exp(jax.random.uniform(key, (CH, NGRID), jnp.float32, 0.0, math.log(10.0)))
    return jnp.clip(base * rise[None, :], 0.01, 10.0).astype(jnp.bfloat16)


def edge_tables(key, capacity, src_rows, dst_rows):
    keys = jax.random.split(key, 6)
    band_ids = jnp.arange(BANDS, dtype=jnp.int32)
    level = jax.random.randint(keys[0], (BANDS, BANDS), 0, 4)
    polar = ((band_ids < max(BANDS // 8, 1)) | (band_ids >= BANDS - max(BANDS // 8, 1))).astype(jnp.int32)
    level = jnp.minimum(level + polar[:, None], 3)
    coins = jax.random.randint(keys[1], (BANDS, BANDS, capacity), 0, 4)
    live = coins <= level[:, :, None]
    full_row = jax.random.randint(keys[2], (), 0, BANDS)
    full_col = jax.random.randint(keys[3], (), 0, BANDS)
    live = live | (band_ids[:, None, None] == full_row) | (band_ids[None, :, None] == full_col)
    source = jax.random.randint(keys[4], (BANDS, BANDS, capacity), 0, src_rows)
    target_ids = jax.random.randint(keys[5], (BANDS, BANDS, capacity), 0, dst_rows)
    sender = jnp.where(live, source, -1).astype(jnp.int32)
    receiver = jnp.transpose(jnp.where(live, target_ids, -1), (1, 0, 2)).astype(jnp.int32)
    return (sender, receiver)


def draw_enc_send(key, part):
    return edge_tables(jax.random.fold_in(key, 11), ENC_CAP, GRID_DEV, MESH_DEV)[0]


def draw_enc_recv(key, part):
    return edge_tables(jax.random.fold_in(key, 11), ENC_CAP, GRID_DEV, MESH_DEV)[1]


def draw_dec_send(key, part):
    return edge_tables(jax.random.fold_in(key, 12), DEC_CAP, MESH_DEV, GRID_DEV)[0]


def draw_dec_recv(key, part):
    return edge_tables(jax.random.fold_in(key, 12), DEC_CAP, MESH_DEV, GRID_DEV)[1]


def shard_levels(own_key, dims, cuts, smallest, high):
    loudness = 1.0
    for dim, parts in cuts:
        steps = jax.random.uniform(jax.random.fold_in(jax.random.fold_in(own_key, 6), dim), (parts,), jnp.float32, smallest / len(cuts), high / len(cuts))
        loudness = loudness * jnp.repeat(jnp.exp(steps), dims[dim] // parts).reshape((-1,) + (1,) * (len(dims) - 1 - dim))
    return loudness


def scatter_about(key, extent, deviation, limit, pieces=(), held_as=jnp.bfloat16):
    factor_of = shard_levels(key, extent, pieces, -0.22, 0.18) if pieces else 1.0
    entries = jax.random.normal(key, extent, jnp.float32) * deviation * factor_of
    return jnp.minimum(jnp.maximum(entries, -limit), limit).astype(held_as)


def setup_inputs(seed: int = 0) -> dict:
    streams_of = jax.random.split(jax.random.key(seed), 14)
    scaled_atmosphere_field = scatter_about(streams_of[0], (CH, NGRID), 1.0, 6.0, ((1, 64),), jnp.float32)
    perturbation = scatter_about(streams_of[1], (MEMBERS, CH, NGRID), 1.0, 6.0, ((0, 8), (2, 64)))
    target = scatter_about(streams_of[2], (MEMBERS, CH, NGRID), 1.0, 6.0, ((0, 8), (2, 64)))
    weight_map = draw_weight_map(jax.random.fold_in(streams_of[13], 71), 0)
    enc_send = draw_enc_send(jax.random.fold_in(streams_of[13], 71), 0)
    enc_recv = draw_enc_recv(jax.random.fold_in(streams_of[13], 71), 0)
    dec_send = draw_dec_send(jax.random.fold_in(streams_of[13], 71), 0)
    dec_recv = draw_dec_recv(jax.random.fold_in(streams_of[13], 71), 0)
    lattice_lift_matrix = scatter_about(streams_of[8], (CH, LAT), CH ** -0.5, 0.625)
    mixing_rescale_factor = jnp.clip(1.0 + 0.18 * jax.random.normal(streams_of[9], (LAT,), jnp.float32), 0.1, 1.9)
    expand_matrix = scatter_about(streams_of[10], (LAT, HID), LAT ** -0.5, 0.25)
    contract_matrix = scatter_about(streams_of[11], (HID, LAT), HID ** -0.5, 0.25)
    readout_matrix = scatter_about(streams_of[12], (LAT, CH), LAT ** -0.5, 0.25)
    return dict(scaled_atmosphere_field=scaled_atmosphere_field, perturbation=perturbation, target=target, weight_map=weight_map, enc_send=enc_send, enc_recv=enc_recv, dec_send=dec_send, dec_recv=dec_recv, lattice_lift_matrix=lattice_lift_matrix, mixing_rescale_factor=mixing_rescale_factor, expand_matrix=expand_matrix, contract_matrix=contract_matrix, readout_matrix=readout_matrix)


smooth_sq = 0.01
norm_eps = 1e-05

def flat_edges(send_table, recv_table, src_rows, dst_rows):
    band_total = send_table.shape[0]
    band_ids = jnp.arange(band_total, dtype=jnp.int32)
    incoming = jnp.transpose(recv_table, (1, 0, 2))
    source = band_ids[:, None, None] * src_rows + jnp.maximum(send_table, 0)
    target_ids = band_ids[None, :, None] * dst_rows + jnp.maximum(incoming, 0)
    live = (send_table >= 0).astype(jnp.float32)
    return (source.reshape(-1).astype(jnp.int32), target_ids.reshape(-1).astype(jnp.int32), live.reshape(-1))

def slope(diff):
    return diff * lax.rsqrt(diff * diff + smooth_sq)

def evaluate_sample_model(scaled_atmosphere_field, noise_one, lattice_lift_matrix, mixing_rescale_factor, expand_matrix, contract_matrix, readout_matrix, intake_link_pairs, readout_link_pairs):
    inputs_b = (scaled_atmosphere_field + noise_one.astype(jnp.float32)).astype(jnp.bfloat16)
    latent = jax.nn.silu(lax.dot_general(inputs_b, lattice_lift_matrix, (((0,), (0,)), ((), ())), preferred_element_type=jnp.float32)).astype(jnp.bfloat16)
    source, target_ids, live = intake_link_pairs
    carried = latent[source].astype(jnp.float32) * live[:, None]
    summed = jax.ops.segment_sum(carried, target_ids, num_segments=NMESH)
    edge_count = jax.ops.segment_sum(live, target_ids, num_segments=NMESH)
    mesh_state = summed / jnp.maximum(edge_count, 1.0)[:, None]
    recip = lax.rsqrt(lax.optimization_barrier(jnp.mean(mesh_state * mesh_state, axis=1, keepdims=True)) + norm_eps)
    normed_b = (mesh_state * recip * mixing_rescale_factor).astype(jnp.bfloat16)
    hidden_pre = jnp.dot(normed_b, expand_matrix, preferred_element_type=jnp.float32)
    hidden_b = jax.nn.silu(hidden_pre).astype(jnp.bfloat16)
    mesh_next = mesh_state + jnp.dot(hidden_b, contract_matrix, preferred_element_type=jnp.float32)
    next_b = mesh_next.astype(jnp.bfloat16)
    projected = jnp.dot(next_b, readout_matrix, preferred_element_type=jnp.float32).astype(jnp.bfloat16)
    dec_source, dec_target, dec_live = readout_link_pairs
    values = projected[dec_source].astype(jnp.float32) * dec_live[:, None]
    grid_sum = jax.ops.segment_sum(values, dec_target, num_segments=NGRID)
    grid_count = jax.ops.segment_sum(dec_live, dec_target, num_segments=NGRID)
    inverse = 1.0 / jnp.maximum(grid_count, 1.0)
    student_outputs = scaled_atmosphere_field + jnp.transpose(grid_sum * inverse[:, None])
    return (student_outputs, (mesh_state, recip, normed_b, hidden_pre, hidden_b, next_b, inverse))

def member_backward(pred_grad, retained_intermediates, mixing_rescale_factor, expand_matrix, contract_matrix, readout_matrix, readout_link_pairs):
    mesh_state, recip, normed_b, hidden_pre, hidden_b, next_b, inverse = retained_intermediates
    highest = lax.Precision.HIGHEST
    scaled = jnp.transpose(pred_grad * inverse[None, :])
    dec_source, dec_target, dec_live = readout_link_pairs
    per_slot = scaled[dec_target] * dec_live[:, None]
    node_grad = jax.ops.segment_sum(per_slot, dec_source, num_segments=NMESH)
    next_grad = jnp.dot(node_grad, jnp.transpose(readout_matrix.astype(jnp.float32)), precision=highest)
    dec_part = jnp.dot(jnp.transpose(next_b.astype(jnp.float32)), node_grad, precision=highest)
    down_part = jnp.dot(jnp.transpose(hidden_b.astype(jnp.float32)), next_grad, precision=highest)
    hidden_grad = jnp.dot(next_grad, jnp.transpose(contract_matrix.astype(jnp.float32)), precision=highest)
    sigma = jax.nn.sigmoid(hidden_pre)
    pre_grad = hidden_grad * sigma * (1.0 + hidden_pre * (1.0 - sigma))
    up_part = jnp.dot(jnp.transpose(normed_b.astype(jnp.float32)), pre_grad, precision=highest)
    normed_grad = jnp.dot(pre_grad, jnp.transpose(expand_matrix.astype(jnp.float32)), precision=highest)
    gain_part = lax.optimization_barrier(jnp.sum(normed_grad * mesh_state * recip, axis=0))
    gained = normed_grad * mixing_rescale_factor
    state_grad = next_grad + recip * gained - mesh_state * (recip * recip * recip) * lax.optimization_barrier(jnp.mean(gained * mesh_state, axis=1, keepdims=True))
    return (state_grad.astype(jnp.bfloat16), up_part, down_part, dec_part, gain_part)

def reference(scaled_atmosphere_field, perturbation, target, weight_map, enc_send, enc_recv, dec_send, dec_recv, lattice_lift_matrix, mixing_rescale_factor, expand_matrix, contract_matrix, readout_matrix):
    intake_link_pairs = flat_edges(enc_send, enc_recv, GRID_DEV, MESH_DEV)
    readout_link_pairs = flat_edges(dec_send, dec_recv, MESH_DEV, GRID_DEV)
    target_f = target.astype(jnp.float32)
    weight_f = weight_map.astype(jnp.float32)
    prediction_pile = []
    savings = []
    for sample_position in range(MEMBERS):
        sample_prediction, retained_intermediates = evaluate_sample_model(scaled_atmosphere_field, perturbation[sample_position], lattice_lift_matrix, mixing_rescale_factor, expand_matrix, contract_matrix, readout_matrix, intake_link_pairs, readout_link_pairs)
        prediction_pile.append(sample_prediction)
        savings.append(retained_intermediates)
    student_outputs = jnp.stack(prediction_pile)
    mesh_grads = []
    collected = ([], [], [], [])
    for sample_position in range(MEMBERS):
        teacher_terms = jnp.zeros_like(student_outputs[sample_position])
        own_terms = jnp.zeros_like(student_outputs[sample_position])
        for other in range(MEMBERS):
            teacher_terms = teacher_terms + slope(student_outputs[sample_position] - target_f[other])
            own_terms = own_terms + slope(student_outputs[sample_position] - student_outputs[other])
        pred_grad = weight_f * (teacher_terms - own_terms)
        state_b, up_part, down_part, dec_part, gain_part = member_backward(pred_grad, savings[sample_position], mixing_rescale_factor, expand_matrix, contract_matrix, readout_matrix, readout_link_pairs)
        mesh_grads.append(state_b)
        for holder, piece in zip(collected, (up_part, down_part, dec_part, gain_part)):
            holder.append(piece)
    factor = 1.0 / math.sqrt(NMESH)
    return (student_outputs, jnp.stack(mesh_grads), jnp.stack(collected[0]) * factor, jnp.stack(collected[1]) * factor, jnp.stack(collected[2]) * factor, jnp.stack(collected[3]) * factor)
```

```python
import functools
import math

import jax
import jax.numpy as jnp
from jax import lax
from jax.experimental import pallas as pl
from jax.experimental.pallas import tpu as pltpu
from jax.sharding import PartitionSpec as P

MESH = pl.DeviceIdType.MESH
BF = jnp.bfloat16
F32 = jnp.float32
NX = 4
PAD = 128
smooth_sq = 0.01
norm_eps = 1e-05


def dot(a, b, ca=1, cb=0):
    return lax.dot_general(a, b, (((ca,), (cb,)), ((), ())), preferred_element_type=F32)


def slope(diff):
    return diff * lax.rsqrt(diff * diff + smooth_sq)


def pad_rows(a, rows):
    return jnp.concatenate([a, jnp.zeros((rows - a.shape[0], a.shape[1]), a.dtype)], axis=0)


def one_hot(table_ref, width):
    bands, cap = table_ref.shape
    slots = bands * cap
    table = table_ref[...].astype(F32).astype(BF)
    row = lax.broadcasted_iota(jnp.int32, (slots, bands), 0)
    col = lax.broadcasted_iota(jnp.int32, (slots, bands), 1)
    owner = jnp.where(row // cap == col, 1.0, 0.0).astype(BF)
    spread = dot(owner, table)
    row = lax.broadcasted_iota(jnp.int32, (slots, cap), 0)
    col = lax.broadcasted_iota(jnp.int32, (slots, cap), 1)
    spread = jnp.where(row % cap == col, spread, 0.0).astype(BF)
    wide = dot(spread, jnp.ones((cap, width), BF))
    lanes = lax.broadcasted_iota(jnp.int32, (slots, width), 1).astype(F32)
    return jnp.where(wide == lanes, 1.0, 0.0)


def step_kernel(
    field, noise, target, weight, enc_send, enc_recv, dec_send, dec_recv,
    lift, mixing, expand, contract, readout,
    stu_out, grad_out, sums_out,
    send1, recv1, send2, recv2, send3, recv3,
    teach, stu, stus, enc_land, dec_pick, dec_land, fill, readp, liftp, both,
    normed_t, hidden_t, next_t, state, hidden_pre, dsilu, grad_b,
    sums, from_x, part, from_z, full,
    s1, r1, s2, r2, s3, r3, st, rt, ss, rs, sx, rx, sz, rz, sg, rg, sh, rh, l1, l2, l3,
):
    bands = send1.shape[0]
    members = teach.shape[0]
    nz = bands // NX
    b = lax.axis_index("band")
    m = lax.axis_index("member")
    z = b // NX
    x = b % NX
    slots = send1.shape[0] * send1.shape[1]
    channels, cells = field.shape
    nodes = cells

    barrier = pltpu.get_barrier_semaphore()

    def greet_band(k, carry):
        pl.semaphore_signal(
            barrier, inc=1, device_id={"band": (b + k) % bands}, device_id_type=MESH
        )
        return carry

    def greet_member(k, carry):
        pl.semaphore_signal(
            barrier, inc=1, device_id={"member": (m + k) % members}, device_id_type=MESH
        )
        return carry

    lax.fori_loop(1, bands, greet_band, 0)
    lax.fori_loop(1, members, greet_member, 0)

    def to_slots(value, ref):
        ref[...] = value.reshape(ref.shape).astype(BF)

    def from_slots(ref):
        return ref[...].astype(F32).reshape(slots, PAD).astype(BF)

    def band_copy(src, dst, ssem, rsem, peer):
        return pltpu.make_async_remote_copy(
            src_ref=src, dst_ref=dst, send_sem=ssem, recv_sem=rsem,
            device_id={"band": peer}, device_id_type=MESH,
        )

    def exchange(send, recv, ssem, rsem):
        def go(k, carry):
            peer = (b + k) % bands
            band_copy(send.at[peer], recv.at[b], ssem, rsem, peer).start()
            return carry

        lax.fori_loop(1, bands, go, 0)
        recv[pl.ds(b, 1)] = send[pl.ds(b, 1)]

    def whole(send, recv, ssem, rsem):
        some = pl.ds(0, bands - 1)
        return band_copy(send.at[some], recv.at[some], ssem, rsem, (b + 1) % bands)

    def member_copy(src, dst, ssem, rsem, peer):
        return pltpu.make_async_remote_copy(
            src_ref=src, dst_ref=dst, send_sem=ssem, recv_sem=rsem,
            device_id={"member": peer}, device_id_type=MESH,
        )

    inputs = pad_rows((field[...] + noise[...].astype(F32)).astype(BF).astype(F32), PAD).astype(BF)
    to_slots(dot(one_hot(enc_send, cells).astype(BF), inputs, 1, 1), send1)
    pl.semaphore_wait(barrier, bands - 1 + members - 1)
    exchange(send1, recv1, s1, r1)

    def send_target(k, carry):
        member_copy(target, teach.at[m], st, rt, (m + k) % members).start()
        return carry

    lax.fori_loop(1, members, send_target, 0)
    teach[pl.ds(m, 1)] = target[...][None]

    land = one_hot(enc_recv, nodes).T
    enc_land[...] = land.astype(BF)
    edge_scale = 1.0 / jnp.maximum(jnp.sum(land, axis=1, keepdims=True), 1.0)
    liftp[...] = pad_rows(lift[...].astype(F32), PAD).astype(BF)
    readp[...] = jnp.zeros(readp.shape, BF)
    readp[:, :channels] = readout[...]
    both[...] = dot(contract[...], readp[...]).astype(BF)
    pick = one_hot(dec_send, nodes)
    dec_pick[...] = pick.astype(BF)
    dec_land[...] = pick.T.astype(BF)
    cover = one_hot(dec_recv, cells)
    fill[...] = cover.astype(BF)
    inverse = 1.0 / jnp.maximum(jnp.sum(cover, axis=0, keepdims=True), 1.0)

    whole(send1, recv1, s1, r1).wait_recv()
    rows = jax.nn.silu(dot(from_slots(recv1), liftp[...])).astype(BF)
    state[...] = dot(enc_land[...], rows) * edge_scale
    recip = lax.rsqrt(jnp.mean(state[...] * state[...], axis=1, keepdims=True) + norm_eps)
    normed = (state[...] * recip * mixing[...]).astype(BF)
    hidden_pre[...] = dot(normed, expand[...])
    hidden = jax.nn.silu(hidden_pre[...]).astype(BF)
    next_b = (state[...] + dot(hidden, contract[...])).astype(BF)
    projected = dot(next_b, readp[...]).astype(BF)
    to_slots(dot(dec_pick[...], projected), send2)
    exchange(send2, recv2, s2, r2)

    normed_t[...] = normed.astype(F32).T.astype(BF)
    hidden_t[...] = hidden.astype(F32).T.astype(BF)
    next_t[...] = next_b.astype(F32).T.astype(BF)
    sigma = jax.nn.sigmoid(hidden_pre[...])
    dsilu[...] = sigma * (1.0 + hidden_pre[...] * (1.0 - sigma))

    def every_target():
        some = pl.ds(0, members - 1)
        return member_copy(teach.at[some], teach.at[some], st, rt, (m + 1) % members)

    every_target().wait_recv()
    whole(send2, recv2, s2, r2).wait_recv()
    grid_sum = dot(from_slots(recv2), fill[...], 0, 0)[:channels]
    mine = field[...] + grid_sum * inverse
    stu[...] = mine

    def send_student(k, carry):
        member_copy(stu, stus.at[m], ss, rs, (m + k) % members).start()
        return carry

    lax.fori_loop(1, members, send_student, 0)
    stu_copy = pltpu.make_async_copy(stu, stu_out, l1)
    stu_copy.start()
    pull = jnp.zeros((channels, cells), F32)
    for j in range(members):
        pull = pull + slope(mine - teach[j].astype(F32))
    some = pl.ds(0, members - 1)
    every_student = member_copy(stus.at[some], stus.at[some], ss, rs, (m + 1) % members)
    every_student.wait_recv()
    for j in range(1, members):
        pull = pull - slope(mine - stus[pl.ds((m + j) % members, 1)][0])
    scaled = weight[...].astype(F32) * pull * inverse
    to_slots(dot(fill[...], pad_rows(scaled, PAD).astype(BF), 1, 1), send3)
    exchange(send3, recv3, s3, r3)
    whole(send3, recv3, s3, r3).wait_recv()

    node_grad = dot(dec_land[...], from_slots(recv3)).astype(BF)
    pre = (dot(node_grad, both[...], 1, 1) * dsilu[...]).astype(BF)
    wide = pre.shape[1]
    blocks = sums.shape[:3]
    sums[:, :, :, :wide] = dot(normed_t[...], pre).reshape(*blocks, wide).astype(BF)
    sums[:, :, :, wide : wide + PAD] = dot(next_t[...], node_grad).reshape(*blocks, PAD).astype(BF)
    sums[:, :, :, wide + PAD :] = dot(hidden_t[...], node_grad).reshape(*blocks, PAD).astype(BF)

    def send_x(k, carry):
        to = (x + k) % NX
        band_copy(sums.at[to], from_x.at[k - 1], sx, rx, z * NX + to).start()
        return carry

    lax.fori_loop(1, NX, send_x, 0)

    next_grad = dot(node_grad, readp[...], 1, 1)
    gained = dot(pre, expand[...], 1, 1) * mixing[...]
    inner = jnp.mean(gained * state[...], axis=1, keepdims=True)
    grad_b[...] = (
        next_grad + recip * gained - state[...] * (recip * recip * recip) * inner
    ).astype(BF)
    grad_copy = pltpu.make_async_copy(grad_b, grad_out, l2)
    grad_copy.start()

    three = pl.ds(0, NX - 1)
    next_x = z * NX + (x + 1) % NX
    every_x = band_copy(sums.at[three], from_x, sx, rx, next_x)
    every_x.wait_recv()
    total = sums[pl.ds(x, 1)][0].astype(F32)
    for k in range(NX - 1):
        total = total + from_x[k].astype(F32)
    part[...] = total.astype(BF)

    def send_z(k, carry):
        to = (z + k) % nz
        band_copy(part.at[to], from_z.at[z], sz, rz, to * NX + x).start()
        return carry

    lax.fori_loop(1, nz, send_z, 0)
    from_z[pl.ds(z, 1)] = part[pl.ds(z, 1)]
    others = pl.ds(0, nz - 1)
    next_z = ((z + 1) % nz) * NX + x
    every_z = band_copy(part.at[others], from_z.at[others], sz, rz, next_z)
    every_z.wait_recv()
    piece = jnp.sum(from_z[...].astype(F32), axis=0).astype(BF)
    full[pl.ds(x, 1), pl.ds(z, 1)] = piece[None, None]

    def gather_z(k, carry):
        to = (z + k) % nz
        band_copy(full.at[x, z], full.at[x, z], sg, rg, to * NX + x).start()
        return carry

    lax.fori_loop(1, nz, gather_z, 0)
    all_z = band_copy(full.at[x, others], full.at[x, others], sg, rg, next_z)
    all_z.wait_recv()

    def gather_x(k, carry):
        band_copy(full.at[x], full.at[x], sh, rh, z * NX + (x + k) % NX).start()
        return carry

    lax.fori_loop(1, NX, gather_x, 0)
    all_x = band_copy(full.at[three], full.at[three], sh, rh, next_x)
    all_x.wait_recv()
    sums_copy = pltpu.make_async_copy(full, sums_out, l3)
    sums_copy.start()

    whole(send1, recv1, s1, r1).wait_send()
    whole(send2, recv2, s2, r2).wait_send()
    whole(send3, recv3, s3, r3).wait_send()
    every_target().wait_send()
    every_student.wait_send()
    every_x.wait_send()
    every_z.wait_send()
    all_z.wait_send()
    all_x.wait_send()
    stu_copy.wait()
    grad_copy.wait()
    sums_copy.wait()


def finish_kernel(factor, sums, mixing, expand, readout, up_out, down_out, dec_out, gain_out):
    rows = sums.shape[0] * sums.shape[1]
    lat, channels = readout.shape
    wide = expand.shape[1]
    flat = sums[...].astype(F32).reshape(rows, sums.shape[2])
    up = flat[:, :wide] * factor
    up_out[...] = up
    dec_out[...] = flat[:, wide : wide + channels] * factor
    hn = flat[:, wide + PAD : wide + PAD + channels].astype(BF)
    down_out[...] = dot(hn, readout[...], 1, 1) * factor
    terms = up * expand[...].astype(F32)
    high = terms.astype(BF)
    low = (terms - high.astype(F32)).astype(BF)
    ones = jnp.ones((8, wide), BF)
    gain = dot(ones, high, 1, 1) + dot(ones, low, 1, 1)
    gain_out[...] = gain[:1] / mixing[...]


def body(
    field, noise, target, weight, enc_send, enc_recv, dec_send, dec_recv,
    lift, mixing, expand, contract, readout,
):
    bands = lax.axis_size("band")
    members = lax.axis_size("member")
    nz = bands // NX
    channels, cells = field.shape
    nodes = cells
    cap = enc_send.shape[2]
    slots = bands * cap
    lat, hid = expand.shape
    wide = hid + 2 * PAD
    vmem = pl.BlockSpec(memory_space=pltpu.VMEM)
    anywhere = pl.BlockSpec(memory_space=pl.ANY)
    blocks = (NX, nz, lat // bands)
    dma = pltpu.SemaphoreType.DMA
    mixing_row = mixing[None]
    slot_buffer = pltpu.VMEM((bands, cap, PAD), BF)
    student, grad, sums = pl.pallas_call(
        step_kernel,
        out_shape=(
            jax.ShapeDtypeStruct((channels, cells), F32),
            jax.ShapeDtypeStruct((nodes, lat), BF),
            jax.ShapeDtypeStruct((*blocks, wide), BF),
        ),
        in_specs=[vmem] * 13,
        out_specs=(anywhere, anywhere, anywhere),
        scratch_shapes=[slot_buffer] * 6
        + [
            pltpu.VMEM((members, channels, cells), BF),
            pltpu.VMEM((channels, cells), F32),
            pltpu.VMEM((members, channels, cells), F32),
            pltpu.VMEM((nodes, slots), BF),
            pltpu.VMEM((slots, nodes), BF),
            pltpu.VMEM((nodes, slots), BF),
            pltpu.VMEM((slots, cells), BF),
            pltpu.VMEM((lat, PAD), BF),
            pltpu.VMEM((PAD, lat), BF),
            pltpu.VMEM((hid, PAD), BF),
            pltpu.VMEM((lat, nodes), BF),
            pltpu.VMEM((hid, nodes), BF),
            pltpu.VMEM((lat, nodes), BF),
            pltpu.VMEM((nodes, lat), F32),
            pltpu.VMEM((nodes, hid), F32),
            pltpu.VMEM((nodes, hid), F32),
            pltpu.VMEM((nodes, lat), BF),
            pltpu.VMEM((*blocks, wide), BF),
            pltpu.VMEM((NX - 1, *blocks[1:], wide), BF),
            pltpu.VMEM((*blocks[1:], wide), BF),
            pltpu.VMEM((*blocks[1:], wide), BF),
            pltpu.VMEM((*blocks, wide), BF),
        ]
        + [dma(())] * 21,
        compiler_params=pltpu.CompilerParams(
            collective_id=0, has_side_effects=True, vmem_limit_bytes=60 << 20
        ),
        name="step",
    )(
        field, noise[0], target[0], weight, enc_send[0], enc_recv[0], dec_send[0], dec_recv[0],
        lift, mixing_row, expand, contract, readout,
    )
    factor = 1.0 / math.sqrt(bands * nodes)
    up, down, dec, gain = pl.pallas_call(
        functools.partial(finish_kernel, factor),
        out_shape=(
            jax.ShapeDtypeStruct((lat, hid), F32),
            jax.ShapeDtypeStruct((hid, lat), F32),
            jax.ShapeDtypeStruct((lat, channels), F32),
            jax.ShapeDtypeStruct((1, lat), F32),
        ),
        in_specs=[vmem] * 4,
        out_specs=(vmem,) * 4,
        name="finish",
    )(sums.reshape(bands, lat // bands, wide), mixing_row, expand, readout)
    return student[None], grad[None], up[None], down[None], dec[None], gain


def solution(mesh):
    return jax.shard_map(
        body,
        mesh=mesh,
        in_specs=(
            P(None, "band"),
            P("member", None, "band"),
            P("member", None, "band"),
            P(None, "band"),
            P("band", None, None),
            P("band", None, None),
            P("band", None, None),
            P("band", None, None),
            P(),
            P(),
            P(),
            P(),
            P(),
        ),
        out_specs=(
            P("member", None, "band"),
            P("member", "band", None),
            P("member", None, None),
            P("member", None, None),
            P("member", None, None),
            P("member", None),
        ),
        check_vma=False,
    )
```

```python
import functools
import math

import jax
import jax.numpy as jnp
from jax import lax
from jax.experimental import pallas as pl
from jax.experimental.pallas import tpu as pltpu
from jax.sharding import PartitionSpec as P

MESH = pl.DeviceIdType.MESH
BF = jnp.bfloat16
F32 = jnp.float32
NX = 4
PAD = 128
smooth_sq = 0.01
norm_eps = 1e-05


def dot(a, b, ca=1, cb=0):
    return lax.dot_general(a, b, (((ca,), (cb,)), ((), ())), preferred_element_type=F32)


def slope(diff):
    return diff * lax.rsqrt(diff * diff + smooth_sq)


def pad_rows(a, rows):
    return jnp.concatenate([a, jnp.zeros((rows - a.shape[0], a.shape[1]), a.dtype)], axis=0)


def one_hot(table_ref, width):
    cap, bands = table_ref.shape
    slots = bands * cap
    table = table_ref[...].astype(F32).astype(BF)
    row = lax.broadcasted_iota(jnp.int32, (slots, bands), 0)
    col = lax.broadcasted_iota(jnp.int32, (slots, bands), 1)
    owner = jnp.where(row // cap == col, 1.0, 0.0).astype(BF)
    spread = dot(owner, table, 1, 1)
    row = lax.broadcasted_iota(jnp.int32, (slots, cap), 0)
    col = lax.broadcasted_iota(jnp.int32, (slots, cap), 1)
    spread = jnp.where(row % cap == col, spread, 0.0).astype(BF)
    wide = dot(spread, jnp.ones((cap, width), BF))
    lanes = lax.broadcasted_iota(jnp.int32, (slots, width), 1).astype(F32)
    return jnp.where(wide == lanes, 1.0, 0.0)


def far_first(j, half):
    return half + (1 - 2 * (j % 2)) * ((j + 1) // 2)


def step_kernel(
    enc_send_in, field_in, noise_in, lift_in, enc_recv_in, dec_send_in, dec_recv_in,
    mixing_in, expand_in, contract_in, readout_in, target_in, weight_in,
    stu_out, grad_out, sums_out,
    enc_send, field, noise, lift, enc_recv, dec_send, dec_recv,
    mixing, expand, contract, readout, target, weight,
    send1, recv1, send2, recv2, send3, recv3,
    teach, stu, stus, enc_land, dec_pick, dec_land, fill, readp, both,
    normed_t, hidden_t, next_t, state, hidden_pre, dsilu, grad_b,
    sums, relay, ahead, from_x, part, from_z, full,
    loads, s1, r1, s2, r2, s3, r3, st, rt, ss, rs, sf, rf,
    s_rel, r_rel, s_x, s_x2, r_x, s_z, r_z, s_gz, r_gz, s_gx, r_gx, s_fw, r_fw, l1, l2, l3,
):
    bands = send1.shape[0]
    members = teach.shape[0]
    nz = bands // NX
    half = nz // 2
    chunks = sums.shape[0]
    b = lax.axis_index("band")
    m = lax.axis_index("member")
    z = b // NX
    x = b % NX
    y = m // 2
    core = m % 2
    slots = send1.shape[0] * send1.shape[1]
    channels, cells = field.shape
    nodes = cells

    into = (
        enc_send, field, noise, lift, enc_recv, dec_send, dec_recv,
        mixing, expand, contract, readout, target, weight,
    )
    out_of = (
        enc_send_in, field_in, noise_in, lift_in, enc_recv_in, dec_send_in, dec_recv_in,
        mixing_in, expand_in, contract_in, readout_in, target_in, weight_in,
    )
    load = [pltpu.make_async_copy(o, i, loads.at[k]) for k, (o, i) in enumerate(zip(out_of, into))]
    for copy in load[:3]:
        copy.start()

    def peer_of(t):
        return ((z + far_first(t // NX, half)) % nz) * NX + (x + NX - 1 - t % NX) % NX

    barrier = pltpu.get_barrier_semaphore()

    def greet_band(t, carry):
        pl.semaphore_signal(barrier, inc=1, device_id={"band": peer_of(t)}, device_id_type=MESH)
        return carry

    def greet_member(k, carry):
        pl.semaphore_signal(
            barrier, inc=1, device_id={"member": (m + k) % members}, device_id_type=MESH
        )
        return carry

    lax.fori_loop(0, bands - 1, greet_band, 0)
    lax.fori_loop(1, members, greet_member, 0)
    for copy in load[3:]:
        copy.start()

    def to_slots(value, ref):
        ref[...] = value.reshape(ref.shape).astype(BF)

    def from_slots(ref):
        return ref[...].astype(F32).reshape(slots, PAD).astype(BF)

    def band_copy(src, dst, ssem, rsem, peer):
        return pltpu.make_async_remote_copy(
            src_ref=src, dst_ref=dst, send_sem=ssem, recv_sem=rsem,
            device_id={"band": peer}, device_id_type=MESH,
        )

    def member_copy(src, dst, ssem, rsem, peer):
        return pltpu.make_async_remote_copy(
            src_ref=src, dst_ref=dst, send_sem=ssem, recv_sem=rsem,
            device_id={"member": peer}, device_id_type=MESH,
        )

    def exchange(send, recv, ssem, rsem):
        def go(t, carry):
            peer = peer_of(t)
            band_copy(send.at[peer], recv.at[b], ssem, rsem, peer).start()
            return carry

        lax.fori_loop(0, bands - 1, go, 0)
        recv[pl.ds(b, 1)] = send[pl.ds(b, 1)]

    def whole(send, recv, ssem, rsem):
        some = pl.ds(0, bands - 1)
        return band_copy(send.at[some], recv.at[some], ssem, rsem, (b + 1) % bands)

    for copy in load[:3]:
        copy.wait()
    inputs = pad_rows((field[...] + noise[...].astype(F32)).astype(BF).astype(F32), PAD).astype(BF)
    to_slots(dot(one_hot(enc_send, cells).astype(BF), inputs, 1, 1), send1)
    pl.semaphore_wait(barrier, bands - 1 + members - 1)
    exchange(send1, recv1, s1, r1)
    for copy in load[3:]:
        copy.wait()

    def send_target(k, carry):
        member_copy(target, teach.at[m], st, rt, (m + k) % members).start()
        return carry

    lax.fori_loop(1, members, send_target, 0)
    teach[pl.ds(m, 1)] = target[...][None]

    land = one_hot(enc_recv, nodes).T
    enc_land[...] = land.astype(BF)
    edge_scale = 1.0 / jnp.maximum(jnp.sum(land, axis=1, keepdims=True), 1.0)
    lift_rows = pad_rows(lift[...].astype(F32), PAD).astype(BF)
    readp[...] = pad_rows(readout[...].astype(F32), PAD).astype(BF)
    both[...] = dot(contract[...], readp[...], 1, 1).astype(BF)
    pick = one_hot(dec_send, nodes)
    dec_pick[...] = pick.astype(BF)
    dec_land[...] = pick.T.astype(BF)
    cover = one_hot(dec_recv, cells)
    fill[...] = cover.astype(BF)
    inverse = 1.0 / jnp.maximum(jnp.sum(cover, axis=0, keepdims=True), 1.0)

    whole(send1, recv1, s1, r1).wait_recv()
    rows = jax.nn.silu(dot(from_slots(recv1), lift_rows)).astype(BF)
    state[...] = dot(enc_land[...], rows) * edge_scale
    recip = lax.rsqrt(jnp.mean(state[...] * state[...], axis=1, keepdims=True) + norm_eps)
    normed = (state[...] * recip * mixing[...]).astype(BF)
    hidden_pre[...] = dot(normed, expand[...])
    hidden = jax.nn.silu(hidden_pre[...]).astype(BF)
    next_b = (state[...] + dot(hidden, contract[...])).astype(BF)
    projected = dot(next_b, readp[...], 1, 1).astype(BF)
    to_slots(dot(dec_pick[...], projected), send2)
    exchange(send2, recv2, s2, r2)

    normed_t[...] = normed.astype(F32).T.astype(BF)
    hidden_t[...] = hidden.astype(F32).T.astype(BF)
    next_t[...] = next_b.astype(F32).T.astype(BF)
    sigma = jax.nn.sigmoid(hidden_pre[...])
    dsilu[...] = sigma * (1.0 + hidden_pre[...] * (1.0 - sigma))

    seven = pl.ds(0, members - 1)
    every_target = member_copy(teach.at[seven], teach.at[seven], st, rt, (m + 1) % members)
    every_target.wait_recv()
    whole(send2, recv2, s2, r2).wait_recv()
    grid_sum = dot(from_slots(recv2), fill[...], 0, 0)[:channels]
    mine = field[...] + grid_sum * inverse
    stu[...] = mine

    chips = members // 2
    partner = y * 2 + 1 - core

    def chip(k):
        return ((y + k) % chips) * 2

    direct = [
        member_copy(stu, stus.at[m], ss.at[k], rs.at[k], chip(k) + core if k else partner)
        for k in range(chips)
    ]
    for k in (2, 1, 3, 0):
        direct[k].start()
    stu_copy = pltpu.make_async_copy(stu, stu_out, l1)
    stu_copy.start()
    pull = jnp.zeros((channels, cells), F32)
    for j in range(members):
        pull = pull + slope(mine - teach[j].astype(F32))
    passed = []
    for k in (0, 1, 3, 2):
        direct[k].wait_recv()
        if k:
            source = chip(chips - k) + core
            copy = member_copy(stus.at[source], stus.at[source], sf.at[k], rf.at[k], partner)
            copy.start()
            passed.append((k, copy))
        else:
            source = partner
        pull = pull - slope(mine - stus[pl.ds(source, 1)][0])
    for k, copy in passed:
        copy.wait_recv()
        pull = pull - slope(mine - stus[pl.ds(chip(chips - k) + 1 - core, 1)][0])
    scaled = weight[...].astype(F32) * pull * inverse
    to_slots(dot(fill[...], pad_rows(scaled, PAD).astype(BF), 1, 1), send3)
    exchange(send3, recv3, s3, r3)
    whole(send3, recv3, s3, r3).wait_recv()

    node_grad = dot(dec_land[...], from_slots(recv3)).astype(BF)
    up_x = z * NX + (x + 1) % NX
    down_x = z * NX + (x + NX - 1) % NX
    right = (x + 1) % NX
    left = (x + NX - 1) % NX
    across = (x + 2) % NX
    low = pl.ds(0, half)
    high = pl.ds(half, half)
    quarter = sums.shape[1:4]
    wide = sums.shape[4]

    def launch(c):
        g = sums.at[c]
        band_copy(g.at[across, low], relay.at[c, 0], s_rel.at[c], r_rel.at[c], up_x).start()
        band_copy(g.at[across, high], relay.at[c, 1], s_rel.at[c], r_rel.at[c], down_x).start()
        band_copy(g.at[right, high], from_x.at[c, 0, high], s_x.at[c], r_x.at[c], up_x).start()
        band_copy(g.at[left, low], from_x.at[c, 1, low], s_x.at[c], r_x.at[c], down_x).start()

    last = chunks - 1
    sums[last, :, :, :, :PAD] = dot(next_t[...], node_grad).reshape(*quarter, PAD).astype(BF)
    sums[last, :, :, :, PAD:] = dot(hidden_t[...], node_grad).reshape(*quarter, PAD).astype(BF)
    launch(last)
    pre = (dot(node_grad, both[...], 1, 1) * dsilu[...]).astype(BF)
    for c in range(last):
        some = pre[:, c * wide : (c + 1) * wide]
        sums[c] = dot(normed_t[...], some).reshape(*quarter, wide).astype(BF)
        launch(c)

    order = [last, *range(last)]
    every_rel = [
        band_copy(relay.at[c], relay.at[c], s_rel.at[c], r_rel.at[c], up_x) for c in range(chunks)
    ]
    for c in order:
        every_rel[c].wait_recv()
        mine_up = sums[c, pl.ds(right, 1), low][0].astype(F32) + relay[c, 0].astype(F32)
        mine_down = sums[c, pl.ds(left, 1), high][0].astype(F32) + relay[c, 1].astype(F32)
        ahead[c, 0] = mine_up.astype(BF)
        ahead[c, 1] = mine_down.astype(BF)
        band_copy(ahead.at[c, 0], from_x.at[c, 0, low], s_x2.at[c], r_x.at[c], up_x).start()
        band_copy(ahead.at[c, 1], from_x.at[c, 1, high], s_x2.at[c], r_x.at[c], down_x).start()

    ring = pl.ds(0, nz - 1)
    next_z = ((z + 1) % nz) * NX + x
    for c in order:
        band_copy(from_x.at[c], from_x.at[c], s_x.at[c], r_x.at[c], up_x).wait_recv()
        total = sums[c, pl.ds(x, 1)][0].astype(F32)
        total = total + from_x[c, 0].astype(F32) + from_x[c, 1].astype(F32)
        part[c] = total.astype(BF)

        def send_z(j, carry, c=c):
            to = (z + far_first(j, half)) % nz
            band_copy(
                part.at[c, to], from_z.at[c, z], s_z.at[c], r_z.at[c], to * NX + x
            ).start()
            return carry

        lax.fori_loop(0, nz - 1, send_z, 0)
        from_z[c, pl.ds(z, 1)] = part[c, pl.ds(z, 1)]

    next_grad = dot(node_grad, readp[...])
    gained = dot(pre, expand[...], 1, 1) * mixing[...]
    inner = jnp.mean(gained * state[...], axis=1, keepdims=True)
    grad_b[...] = (
        next_grad + recip * gained - state[...] * (recip * recip * recip) * inner
    ).astype(BF)
    grad_copy = pltpu.make_async_copy(grad_b, grad_out, l2)
    grad_copy.start()

    every_z = [
        band_copy(from_z.at[c, ring], from_z.at[c, ring], s_z.at[c], r_z.at[c], next_z)
        for c in range(chunks)
    ]
    all_z = [
        band_copy(full.at[c, x, ring], full.at[c, x, ring], s_gz.at[c], r_gz.at[c], next_z)
        for c in range(chunks)
    ]
    for c in order:
        every_z[c].wait_recv()
        piece = jnp.sum(from_z[c].astype(F32), axis=0).astype(BF)
        full[c, pl.ds(x, 1), pl.ds(z, 1)] = piece[None, None]

        def gather_z(j, carry, c=c):
            to = (z + far_first(j, half)) % nz
            mine_z = full.at[c, x, z]
            band_copy(mine_z, mine_z, s_gz.at[c], r_gz.at[c], to * NX + x).start()
            return carry

        lax.fori_loop(0, nz - 1, gather_z, 0)

    gx = []
    for c in order:
        all_z[c].wait_recv()
        mine_x = full.at[c, x]
        pair = (
            band_copy(mine_x, mine_x, s_gx.at[c, 0], r_gx.at[c, 0], up_x),
            band_copy(mine_x, mine_x, s_gx.at[c, 1], r_gx.at[c, 1], down_x),
        )
        for copy in pair:
            copy.start()
        gx.append(pair)
    fw = []
    for c, pair in zip(order, gx):
        pair[0].wait_recv()
        there = full.at[c, left, low]
        band_copy(there, there, s_fw.at[c], r_fw.at[c], up_x).start()
        pair[1].wait_recv()
        there = full.at[c, right, high]
        band_copy(there, there, s_fw.at[c], r_fw.at[c], down_x).start()
        fw.append(band_copy(full.at[c, across], full.at[c, across], s_fw.at[c], r_fw.at[c], up_x))
    sums_copies = []
    for c, copy in zip(order, fw):
        copy.wait_recv()
        sums_copies.append(pltpu.make_async_copy(full.at[c], sums_out.at[c], l3.at[c]))
        sums_copies[-1].start()

    whole(send1, recv1, s1, r1).wait_send()
    whole(send2, recv2, s2, r2).wait_send()
    whole(send3, recv3, s3, r3).wait_send()
    every_target.wait_send()
    for copy in direct:
        copy.wait_send()
    for k, copy in passed:
        copy.wait_send()
    for i, c in enumerate(order):
        every_rel[c].wait_send()
        band_copy(sums.at[c, 0], sums.at[c, 0], s_x.at[c], r_x.at[c], up_x).wait_send()
        band_copy(ahead.at[c], ahead.at[c], s_x2.at[c], r_x.at[c], up_x).wait_send()
        every_z[c].wait_send()
        all_z[c].wait_send()
        for copy in gx[i]:
            copy.wait_send()
        fw[i].wait_send()
    stu_copy.wait()
    grad_copy.wait()
    for copy in sums_copies:
        copy.wait()


def finish_kernel(
    factor, sums, mixing, expand, readout, stu_in, grad_in,
    up_out, down_out, dec_out, gain_out, stu_out, grad_out,
    up, down, dec, stu, grad, sems,
):
    chunks, pieces, depth, wide = sums.shape
    rows = pieces * depth
    lat = expand.shape[1]
    channels = readout.shape[0]
    ins = [
        pltpu.make_async_copy(stu_in, stu, sems.at[0]),
        pltpu.make_async_copy(grad_in, grad, sems.at[1]),
    ]
    for copy in ins:
        copy.start()
    low = sums[chunks - 1].astype(F32).reshape(rows, wide)
    outs = []

    def send(src, dst):
        outs.append(pltpu.make_async_copy(src, dst, sems.at[2 + len(outs)]))
        outs[-1].start()

    for c in range(chunks - 1):
        up[:, c * wide : (c + 1) * wide] = sums[c].astype(F32).reshape(rows, wide) * factor
    send(up, up_out)
    read_rows = pad_rows(readout[...].astype(F32), PAD).astype(BF)
    down[...] = dot(low[:, PAD:].astype(BF), read_rows) * factor
    send(down, down_out)
    dec[...] = low[:, :PAD].T[:channels] * factor
    send(dec, dec_out)
    for copy in ins:
        copy.wait()
    send(stu, stu_out)
    send(grad, grad_out)
    terms = up[...] * expand[...].astype(F32)
    high = terms.astype(BF)
    rest = (terms - high.astype(F32)).astype(BF)
    ones = jnp.ones((8, lat), BF)
    gain = dot(ones, high, 1, 1) + dot(ones, rest, 1, 1)
    gain_out[...] = gain[:1] / mixing[...]
    for copy in outs:
        copy.wait()


CHUNK = 256


def body(
    field, noise, target, weight, enc_send, enc_recv, dec_send, dec_recv,
    lift, mixing, expand, contract, readout,
):
    bands = lax.axis_size("band")
    members = lax.axis_size("member")
    nz = bands // NX
    channels, cells = field.shape
    nodes = cells
    cap = enc_send.shape[2]
    slots = bands * cap
    lat, hid = expand.shape
    chunks = (hid + 2 * PAD) // CHUNK
    vmem = pl.BlockSpec(memory_space=pltpu.VMEM)
    anywhere = pl.BlockSpec(memory_space=pl.ANY)
    quarter = (nz, lat // bands, CHUNK)
    half = (nz // 2, lat // bands, CHUNK)
    dma = pltpu.SemaphoreType.DMA
    mixing_row = mixing[None]
    read_t = readout.T
    slot_buffer = pltpu.VMEM((bands, cap, PAD), BF)
    ins = (
        enc_send[0].T, field, noise[0], lift, enc_recv[0].T, dec_send[0].T, dec_recv[0].T,
        mixing_row, expand, contract, read_t, target[0], weight,
    )
    student, grad, sums = pl.pallas_call(
        step_kernel,
        out_shape=(
            jax.ShapeDtypeStruct((channels, cells), F32),
            jax.ShapeDtypeStruct((nodes, lat), BF),
            jax.ShapeDtypeStruct((chunks, NX, *quarter), BF),
        ),
        in_specs=[anywhere] * len(ins),
        out_specs=(anywhere, anywhere, anywhere),
        scratch_shapes=[pltpu.VMEM(a.shape, a.dtype) for a in ins]
        + [slot_buffer] * 6
        + [
            pltpu.VMEM((members, channels, cells), BF),
            pltpu.VMEM((channels, cells), F32),
            pltpu.VMEM((members, channels, cells), F32),
            pltpu.VMEM((nodes, slots), BF),
            pltpu.VMEM((slots, nodes), BF),
            pltpu.VMEM((nodes, slots), BF),
            pltpu.VMEM((slots, cells), BF),
            pltpu.VMEM((PAD, lat), BF),
            pltpu.VMEM((hid, PAD), BF),
            pltpu.VMEM((lat, nodes), BF),
            pltpu.VMEM((hid, nodes), BF),
            pltpu.VMEM((lat, nodes), BF),
            pltpu.VMEM((nodes, lat), F32),
            pltpu.VMEM((nodes, hid), F32),
            pltpu.VMEM((nodes, hid), F32),
            pltpu.VMEM((nodes, lat), BF),
            pltpu.VMEM((chunks, NX, *quarter), BF),
            pltpu.VMEM((chunks, 2, *half), BF),
            pltpu.VMEM((chunks, 2, *half), BF),
            pltpu.VMEM((chunks, 2, *quarter), BF),
            pltpu.VMEM((chunks, *quarter), BF),
            pltpu.VMEM((chunks, *quarter), BF),
            pltpu.VMEM((chunks, NX, *quarter), BF),
        ]
        + [dma((len(ins),))]
        + [dma(())] * 8
        + [dma((members // 2,))] * 4
        + [dma((chunks,))] * 9
        + [dma((chunks, 2))] * 2
        + [dma((chunks,))] * 2
        + [dma(()), dma(()), dma((chunks,))],
        compiler_params=pltpu.CompilerParams(
            collective_id=0, has_side_effects=True, vmem_limit_bytes=60 << 20
        ),
        name="step",
    )(*ins)
    factor = 1.0 / math.sqrt(bands * nodes)
    outs = (
        jax.ShapeDtypeStruct((lat, hid), F32),
        jax.ShapeDtypeStruct((hid, lat), F32),
        jax.ShapeDtypeStruct((channels, lat), F32),
        jax.ShapeDtypeStruct((1, lat), F32),
        jax.ShapeDtypeStruct((channels, cells), F32),
        jax.ShapeDtypeStruct((nodes, lat), BF),
    )
    up, down, dec, gain, student, grad = pl.pallas_call(
        functools.partial(finish_kernel, factor),
        out_shape=outs,
        in_specs=[vmem] * 4 + [anywhere] * 2,
        out_specs=(anywhere, anywhere, anywhere, vmem, anywhere, anywhere),
        scratch_shapes=[pltpu.VMEM(outs[i].shape, outs[i].dtype) for i in (0, 1, 2, 4, 5)]
        + [dma((7,))],
        name="finish",
    )(sums.reshape(chunks, bands, lat // bands, CHUNK), mixing_row, expand, read_t, student, grad)
    return student[None], grad[None], up[None], down[None], dec.T[None], gain


def solution(mesh):
    return jax.shard_map(
        body,
        mesh=mesh,
        in_specs=(
            P(None, "band"),
            P("member", None, "band"),
            P("member", None, "band"),
            P(None, "band"),
            P("band", None, None),
            P("band", None, None),
            P("band", None, None),
            P("band", None, None),
            P(),
            P(),
            P(),
            P(),
            P(),
        ),
        out_specs=(
            P("member", None, "band"),
            P("member", "band", None),
            P("member", None, None),
            P("member", None, None),
            P("member", None, None),
            P("member", None),
        ),
        check_vma=False,
    )
```

```python
import functools
import math

import jax
import jax.numpy as jnp
from jax import lax
from jax.experimental import pallas as pl
from jax.experimental.pallas import tpu as pltpu
from jax.sharding import PartitionSpec as P

MESH = pl.DeviceIdType.MESH
BF = jnp.bfloat16
F32 = jnp.float32
NX = 4
PAD = 128
smooth_sq = 0.01
norm_eps = 1e-05


def dot(a, b, ca=1, cb=0):
    return lax.dot_general(a, b, (((ca,), (cb,)), ((), ())), preferred_element_type=F32)


def slope(diff):
    return diff * lax.rsqrt(diff * diff + smooth_sq)


def pad_rows(a, rows):
    return jnp.concatenate([a, jnp.zeros((rows - a.shape[0], a.shape[1]), a.dtype)], axis=0)


def one_hot(table_ref, width):
    cap, bands = table_ref.shape
    slots = bands * cap
    table = table_ref[...].astype(F32).astype(BF)
    row = lax.broadcasted_iota(jnp.int32, (slots, bands), 0)
    col = lax.broadcasted_iota(jnp.int32, (slots, bands), 1)
    owner = jnp.where(row // cap == col, 1.0, 0.0).astype(BF)
    spread = dot(owner, table, 1, 1)
    row = lax.broadcasted_iota(jnp.int32, (slots, cap), 0)
    col = lax.broadcasted_iota(jnp.int32, (slots, cap), 1)
    spread = jnp.where(row % cap == col, spread, 0.0).astype(BF)
    wide = dot(spread, jnp.ones((cap, width), BF))
    lanes = lax.broadcasted_iota(jnp.int32, (slots, width), 1).astype(F32)
    return jnp.where(wide == lanes, 1.0, 0.0)


def far_first(j, half):
    return half + (1 - 2 * (j % 2)) * ((j + 1) // 2)


def step_kernel(
    factor, enc_send_in, field_in, noise_in, lift_in, enc_recv_in, dec_send_in, dec_recv_in,
    mixing_in, expand_in, contract_in, readout_in, target_in, weight_in,
    stu, grad_b, up_out, down_out, dec_out, gain_out,
    enc_send, field, noise, lift, enc_recv, dec_send, dec_recv,
    mixing, expand, contract, readout, target, weight,
    send1, recv1, send2, recv2, send3, recv3,
    teach, stus, enc_land, dec_pick, dec_land, fill, readp, both,
    normed_t, hidden_t, next_t, state, hidden_pre, dsilu,
    sums, from_x, part, from_z, full,
    loads, s1, r1, s2, r2, s3, r3, st, rt, ss, rs, sf, rf,
    s_x, r_x, s_z, r_z, s_gz, r_gz, s_gx, r_gx,
):
    bands = send1.shape[0]
    members = teach.shape[0]
    nz = bands // NX
    half = nz // 2
    chunks = sums.shape[0]
    b = lax.axis_index("band")
    m = lax.axis_index("member")
    z = b // NX
    x = b % NX
    y = m // 2
    core = m % 2
    slots = send1.shape[0] * send1.shape[1]
    channels, cells = field.shape
    nodes = cells

    into = (
        enc_send, field, noise, lift, enc_recv, dec_send, dec_recv,
        mixing, expand, contract, readout, target, weight,
    )
    out_of = (
        enc_send_in, field_in, noise_in, lift_in, enc_recv_in, dec_send_in, dec_recv_in,
        mixing_in, expand_in, contract_in, readout_in, target_in, weight_in,
    )
    load = [pltpu.make_async_copy(o, i, loads.at[k]) for k, (o, i) in enumerate(zip(out_of, into))]
    for copy in load[:3]:
        copy.start()

    def peer_of(t):
        return ((z + far_first(t // NX, half)) % nz) * NX + (x + NX - 1 - t % NX) % NX

    barrier = pltpu.get_barrier_semaphore()

    def greet_band(t, carry):
        pl.semaphore_signal(barrier, inc=1, device_id={"band": peer_of(t)}, device_id_type=MESH)
        return carry

    def greet_member(k, carry):
        pl.semaphore_signal(
            barrier, inc=1, device_id={"member": (m + k) % members}, device_id_type=MESH
        )
        return carry

    lax.fori_loop(0, bands - 1, greet_band, 0)
    lax.fori_loop(1, members, greet_member, 0)
    for copy in load[3:]:
        copy.start()

    def to_slots(value, ref):
        ref[...] = value.reshape(ref.shape).astype(BF)

    def from_slots(ref):
        return ref[...].astype(F32).reshape(slots, PAD).astype(BF)

    def band_copy(src, dst, ssem, rsem, peer):
        return pltpu.make_async_remote_copy(
            src_ref=src, dst_ref=dst, send_sem=ssem, recv_sem=rsem,
            device_id={"band": peer}, device_id_type=MESH,
        )

    def member_copy(src, dst, ssem, rsem, peer):
        return pltpu.make_async_remote_copy(
            src_ref=src, dst_ref=dst, send_sem=ssem, recv_sem=rsem,
            device_id={"member": peer}, device_id_type=MESH,
        )

    def exchange(send, recv, ssem, rsem):
        def go(t, carry):
            peer = peer_of(t)
            band_copy(send.at[peer], recv.at[b], ssem, rsem, peer).start()
            return carry

        lax.fori_loop(0, bands - 1, go, 0)
        recv[pl.ds(b, 1)] = send[pl.ds(b, 1)]

    def whole(send, recv, ssem, rsem):
        some = pl.ds(0, bands - 1)
        return band_copy(send.at[some], recv.at[some], ssem, rsem, (b + 1) % bands)

    for copy in load[:3]:
        copy.wait()
    inputs = pad_rows((field[...] + noise[...].astype(F32)).astype(BF).astype(F32), PAD).astype(BF)
    to_slots(dot(one_hot(enc_send, cells).astype(BF), inputs, 1, 1), send1)
    pl.semaphore_wait(barrier, bands - 1 + members - 1)
    exchange(send1, recv1, s1, r1)
    for copy in load[3:]:
        copy.wait()

    def send_target(k, carry):
        member_copy(target, teach.at[m], st, rt, (m + k) % members).start()
        return carry

    lax.fori_loop(1, members, send_target, 0)
    teach[pl.ds(m, 1)] = target[...][None]

    land = one_hot(enc_recv, nodes).T
    enc_land[...] = land.astype(BF)
    edge_scale = 1.0 / jnp.maximum(jnp.sum(land, axis=1, keepdims=True), 1.0)
    lift_rows = pad_rows(lift[...].astype(F32), PAD).astype(BF)
    readp[...] = pad_rows(readout[...].astype(F32), PAD).astype(BF)
    both[...] = dot(contract[...], readp[...], 1, 1).astype(BF)
    pick = one_hot(dec_send, nodes)
    dec_pick[...] = pick.astype(BF)
    dec_land[...] = pick.T.astype(BF)
    cover = one_hot(dec_recv, cells)
    fill[...] = cover.astype(BF)
    inverse = 1.0 / jnp.maximum(jnp.sum(cover, axis=0, keepdims=True), 1.0)

    whole(send1, recv1, s1, r1).wait_recv()
    rows = jax.nn.silu(dot(from_slots(recv1), lift_rows)).astype(BF)
    state[...] = dot(enc_land[...], rows) * edge_scale
    recip = lax.rsqrt(jnp.mean(state[...] * state[...], axis=1, keepdims=True) + norm_eps)
    normed = (state[...] * recip * mixing[...]).astype(BF)
    hidden_pre[...] = dot(normed, expand[...])
    hidden = jax.nn.silu(hidden_pre[...]).astype(BF)
    next_b = (state[...] + dot(hidden, contract[...])).astype(BF)
    projected = dot(next_b, readp[...], 1, 1).astype(BF)
    to_slots(dot(dec_pick[...], projected), send2)
    exchange(send2, recv2, s2, r2)

    normed_t[...] = normed.astype(F32).T.astype(BF)
    hidden_t[...] = hidden.astype(F32).T.astype(BF)
    next_t[...] = next_b.astype(F32).T.astype(BF)
    sigma = jax.nn.sigmoid(hidden_pre[...])
    dsilu[...] = sigma * (1.0 + hidden_pre[...] * (1.0 - sigma))

    seven = pl.ds(0, members - 1)
    every_target = member_copy(teach.at[seven], teach.at[seven], st, rt, (m + 1) % members)
    every_target.wait_recv()
    whole(send2, recv2, s2, r2).wait_recv()
    grid_sum = dot(from_slots(recv2), fill[...], 0, 0)[:channels]
    mine = field[...] + grid_sum * inverse
    stu[...] = mine

    chips = members // 2
    partner = y * 2 + 1 - core

    def chip(k):
        return ((y + k) % chips) * 2

    direct = [
        member_copy(stu, stus.at[m], ss.at[k], rs.at[k], chip(k) + core if k else partner)
        for k in range(chips)
    ]
    for k in (2, 1, 3, 0):
        direct[k].start()
    pull = jnp.zeros((channels, cells), F32)
    for j in range(members):
        pull = pull + slope(mine - teach[j].astype(F32))
    passed = []
    for k in (0, 1, 3, 2):
        direct[k].wait_recv()
        if k:
            source = chip(chips - k) + core
            copy = member_copy(stus.at[source], stus.at[source], sf.at[k], rf.at[k], partner)
            copy.start()
            passed.append((k, copy))
        else:
            source = partner
        pull = pull - slope(mine - stus[pl.ds(source, 1)][0])
    for k, copy in passed:
        copy.wait_recv()
        pull = pull - slope(mine - stus[pl.ds(chip(chips - k) + 1 - core, 1)][0])
    scaled = weight[...].astype(F32) * pull * inverse
    to_slots(dot(fill[...], pad_rows(scaled, PAD).astype(BF), 1, 1), send3)
    exchange(send3, recv3, s3, r3)
    whole(send3, recv3, s3, r3).wait_recv()

    node_grad = dot(dec_land[...], from_slots(recv3)).astype(BF)
    quarter = sums.shape[1:4]
    wide = sums.shape[4]
    three = pl.ds(0, NX - 1)
    next_x = z * NX + (x + 1) % NX
    far_x = (2, 1, 3)

    def launch(c):
        for k in far_x:
            to = (x + k) % NX
            band_copy(
                sums.at[c, to], from_x.at[c, k - 1], s_x.at[c], r_x.at[c], z * NX + to
            ).start()

    last = chunks - 1
    sums[last, :, :, :, :PAD] = dot(next_t[...], node_grad).reshape(*quarter, PAD).astype(BF)
    sums[last, :, :, :, PAD:] = dot(hidden_t[...], node_grad).reshape(*quarter, PAD).astype(BF)
    launch(last)
    pre = (dot(node_grad, both[...], 1, 1) * dsilu[...]).astype(BF)
    for c in range(last):
        some = pre[:, c * wide : (c + 1) * wide]
        sums[c] = dot(normed_t[...], some).reshape(*quarter, wide).astype(BF)
        launch(c)

    order = [last, *range(last)]
    every_x = [
        band_copy(sums.at[c, three], from_x.at[c], s_x.at[c], r_x.at[c], next_x)
        for c in range(chunks)
    ]
    ring = pl.ds(0, nz - 1)
    next_z = ((z + 1) % nz) * NX + x
    for c in order:
        every_x[c].wait_recv()
        total = sums[c, pl.ds(x, 1)][0].astype(F32)
        for k in range(NX - 1):
            total = total + from_x[c, k].astype(F32)
        part[c] = total.astype(BF)

        def send_z(j, carry, c=c):
            to = (z + far_first(j, half)) % nz
            band_copy(
                part.at[c, to], from_z.at[c, z], s_z.at[c], r_z.at[c], to * NX + x
            ).start()
            return carry

        lax.fori_loop(0, nz - 1, send_z, 0)
        from_z[c, pl.ds(z, 1)] = part[c, pl.ds(z, 1)]

    next_grad = dot(node_grad, readp[...])
    gained = dot(pre, expand[...], 1, 1) * mixing[...]
    inner = jnp.mean(gained * state[...], axis=1, keepdims=True)
    grad_b[...] = (
        next_grad + recip * gained - state[...] * (recip * recip * recip) * inner
    ).astype(BF)

    every_z = [
        band_copy(from_z.at[c, ring], from_z.at[c, ring], s_z.at[c], r_z.at[c], next_z)
        for c in range(chunks)
    ]
    all_z = [
        band_copy(full.at[c, x, ring], full.at[c, x, ring], s_gz.at[c], r_gz.at[c], next_z)
        for c in range(chunks)
    ]
    for c in order:
        every_z[c].wait_recv()
        piece = jnp.sum(from_z[c].astype(F32), axis=0).astype(BF)
        full[c, pl.ds(x, 1), pl.ds(z, 1)] = piece[None, None]

        def gather_z(j, carry, c=c):
            to = (z + far_first(j, half)) % nz
            mine_z = full.at[c, x, z]
            band_copy(mine_z, mine_z, s_gz.at[c], r_gz.at[c], to * NX + x).start()
            return carry

        lax.fori_loop(0, nz - 1, gather_z, 0)

    all_x = [
        band_copy(full.at[c, three], full.at[c, three], s_gx.at[c], r_gx.at[c], next_x)
        for c in range(chunks)
    ]
    for c in order:
        all_z[c].wait_recv()
        for k in far_x:
            mine_x = full.at[c, x]
            band_copy(mine_x, mine_x, s_gx.at[c], r_gx.at[c], z * NX + (x + k) % NX).start()

    rows = quarter[0] * quarter[1] * quarter[2]
    ones = jnp.ones((8, wide), BF)
    gain = jnp.zeros((8, rows), F32)
    for c in order:
        all_x[c].wait_recv()
        some = full[c].astype(F32).reshape(rows, wide)
        if c == last:
            down_out[...] = dot(some[:, PAD:].astype(BF), readp[...]) * factor
            dec_out[...] = some[:, :PAD].T[:channels] * factor
        else:
            at = slice(c * wide, (c + 1) * wide)
            some = some * factor
            up_out[:, at] = some
            terms = some * expand[:, at].astype(F32)
            main = terms.astype(BF)
            rest = (terms - main.astype(F32)).astype(BF)
            gain = gain + dot(ones, main, 1, 1) + dot(ones, rest, 1, 1)
    gain_out[...] = gain[:1] / mixing[...]

    whole(send1, recv1, s1, r1).wait_send()
    whole(send2, recv2, s2, r2).wait_send()
    whole(send3, recv3, s3, r3).wait_send()
    every_target.wait_send()
    for copy in direct:
        copy.wait_send()
    for k, copy in passed:
        copy.wait_send()
    for c in order:
        every_x[c].wait_send()
        every_z[c].wait_send()
        all_z[c].wait_send()
        all_x[c].wait_send()


def write_kernel(*refs):
    sems = refs[-1]
    count = len(refs) // 2
    copies = [pltpu.make_async_copy(refs[k], refs[count + k], sems.at[k]) for k in range(count)]
    for copy in copies:
        copy.start()
    for copy in copies:
        copy.wait()


CHUNK = 256


def body(
    field, noise, target, weight, enc_send, enc_recv, dec_send, dec_recv,
    lift, mixing, expand, contract, readout,
):
    bands = lax.axis_size("band")
    members = lax.axis_size("member")
    nz = bands // NX
    channels, cells = field.shape
    nodes = cells
    cap = enc_send.shape[2]
    slots = bands * cap
    lat, hid = expand.shape
    chunks = (hid + 2 * PAD) // CHUNK
    vmem = pl.BlockSpec(memory_space=pltpu.VMEM)
    hbm = pl.BlockSpec(memory_space=pltpu.HBM)
    quarter = (nz, lat // bands, CHUNK)
    dma = pltpu.SemaphoreType.DMA
    mixing_row = mixing[None]
    read_t = readout.T
    slot_buffer = pltpu.VMEM((bands, cap, PAD), BF)
    ins = (
        enc_send[0].T, field, noise[0], lift, enc_recv[0].T, dec_send[0].T, dec_recv[0].T,
        mixing_row, expand, contract, read_t, target[0], weight,
    )
    factor = 1.0 / math.sqrt(bands * nodes)
    results = pl.pallas_call(
        functools.partial(step_kernel, factor),
        out_shape=(
            pltpu.VMEM((channels, cells), F32),
            pltpu.VMEM((nodes, lat), BF),
            pltpu.VMEM((lat, hid), F32),
            pltpu.VMEM((hid, lat), F32),
            pltpu.VMEM((channels, lat), F32),
            pltpu.VMEM((1, lat), F32),
        ),
        in_specs=[hbm] * len(ins),
        out_specs=(vmem,) * 6,
        scratch_shapes=[pltpu.VMEM(a.shape, a.dtype) for a in ins]
        + [slot_buffer] * 6
        + [
            pltpu.VMEM((members, channels, cells), BF),
            pltpu.VMEM((members, channels, cells), F32),
            pltpu.VMEM((nodes, slots), BF),
            pltpu.VMEM((slots, nodes), BF),
            pltpu.VMEM((nodes, slots), BF),
            pltpu.VMEM((slots, cells), BF),
            pltpu.VMEM((PAD, lat), BF),
            pltpu.VMEM((hid, PAD), BF),
            pltpu.VMEM((lat, nodes), BF),
            pltpu.VMEM((hid, nodes), BF),
            pltpu.VMEM((lat, nodes), BF),
            pltpu.VMEM((nodes, lat), F32),
            pltpu.VMEM((nodes, hid), F32),
            pltpu.VMEM((nodes, hid), F32),
            pltpu.VMEM((chunks, NX, *quarter), BF),
            pltpu.VMEM((chunks, NX - 1, *quarter), BF),
            pltpu.VMEM((chunks, *quarter), BF),
            pltpu.VMEM((chunks, *quarter), BF),
            pltpu.VMEM((chunks, NX, *quarter), BF),
        ]
        + [dma((len(ins),))]
        + [dma(())] * 8
        + [dma((members // 2,))] * 4
        + [dma((chunks,))] * 8,
        compiler_params=pltpu.CompilerParams(
            collective_id=0, has_side_effects=True, vmem_limit_bytes=40 << 20
        ),
        name="step",
    )(*(pltpu.with_memory_space_constraint(a, pltpu.HBM) for a in ins))
    student, grad, up, down, dec, gain = pl.pallas_call(
        write_kernel,
        out_shape=tuple(jax.ShapeDtypeStruct(a.shape, a.dtype) for a in results),
        in_specs=[vmem] * 6,
        out_specs=(hbm,) * 6,
        scratch_shapes=[dma((6,))],
        name="write",
    )(*(pltpu.with_memory_space_constraint(a, pltpu.VMEM) for a in results))
    return student[None], grad[None], up[None], down[None], dec.T[None], gain


def solution(mesh):
    return jax.shard_map(
        body,
        mesh=mesh,
        in_specs=(
            P(None, "band"),
            P("member", None, "band"),
            P("member", None, "band"),
            P(None, "band"),
            P("band", None, None),
            P("band", None, None),
            P("band", None, None),
            P("band", None, None),
            P(),
            P(),
            P(),
            P(),
            P(),
        ),
        out_specs=(
            P("member", None, "band"),
            P("member", "band", None),
            P("member", None, None),
            P("member", None, None),
            P("member", None, None),
            P("member", None),
        ),
        check_vma=False,
    )
```

```python
import functools
import math

import jax
import jax.numpy as jnp
from jax import lax
from jax.experimental import pallas as pl
from jax.experimental.pallas import tpu as pltpu
from jax.sharding import PartitionSpec as P

MESH = pl.DeviceIdType.MESH
BF = jnp.bfloat16
F32 = jnp.float32
NX = 4
PAD = 128
CHUNKS = (("down", 0, 128), ("dec", 0, 128), ("up", 0, 128), ("up", 128, 128), ("up", 256, 128), ("up", 384, 128))
smooth_sq = 0.01
norm_eps = 1e-05


def dot(a, b, ca=1, cb=0):
    return lax.dot_general(a, b, (((ca,), (cb,)), ((), ())), preferred_element_type=F32)


def slope(diff):
    return diff * lax.rsqrt(diff * diff + smooth_sq)


def sigmoid(v):
    return 0.5 + 0.5 * jnp.tanh(0.5 * v)


def pad_rows(a, rows):
    return jnp.concatenate([a, jnp.zeros((rows - a.shape[0], a.shape[1]), a.dtype)], axis=0)


def one_hot(table_ref, width):
    cap, bands = table_ref.shape
    slots = bands * cap
    table = table_ref[...].astype(F32).astype(BF)
    row = lax.broadcasted_iota(jnp.int32, (slots, bands), 0)
    col = lax.broadcasted_iota(jnp.int32, (slots, bands), 1)
    owner = jnp.where(row // cap == col, 1.0, 0.0).astype(BF)
    spread = dot(owner, table, 1, 1)
    row = lax.broadcasted_iota(jnp.int32, (slots, cap), 0)
    col = lax.broadcasted_iota(jnp.int32, (slots, cap), 1)
    spread = jnp.where(row % cap == col, spread, 0.0).astype(BF)
    wide = dot(spread, jnp.ones((cap, width), BF))
    lanes = lax.broadcasted_iota(jnp.int32, (slots, width), 1).astype(F32)
    return jnp.where(wide == lanes, 1.0, 0.0)


def far_first(j, half):
    return half + (1 - 2 * (j % 2)) * ((j + 1) // 2)


def step_kernel(
    factor, enc_send_in, field_in, noise_in, lift_in, enc_recv_in, dec_send_in, dec_recv_in,
    mixing_in, expand_in, contract_in, readout_in, target_in, weight_in,
    stu, grad_b, up_out, down_out, dec_out, gain_out,
    enc_send, field, noise, lift, enc_recv, dec_send, dec_recv,
    mixing, expand, contract, readout, target, weight,
    send1, recv1, send2, recv2, send3, recv3,
    teach, halves_b, halves, stus, weights, inverses, pieces, enc_land, dec_pick, dec_land, fill, readp, both,
    normed_t, hidden_t, next_t, state, hidden_pre, dsilu,
    loads, s1, r1, s2, r2, s3, r3, st, rt, ss, rs, sp, rp,
    s_x, r_x, s_z, r_z, s_gz, r_gz, s_gx, r_gx, *chunk_refs,
):
    bands = send1.shape[0]
    members = teach.shape[0]
    nz = bands // NX
    half = nz // 2
    chunks = len(CHUNKS)
    sums, from_x, part, from_z, full = (chunk_refs[k * chunks : (k + 1) * chunks] for k in range(5))
    b = lax.axis_index("band")
    m = lax.axis_index("member")
    z = b // NX
    x = b % NX
    y = m // 2
    core = m % 2
    slots = send1.shape[0] * send1.shape[1]
    channels, cells = field.shape
    nodes = cells
    cut = cells // 2

    into = (
        enc_send, field, noise, lift, enc_recv, dec_send, dec_recv,
        mixing, expand, contract, readout, target, weight,
    )
    out_of = (
        enc_send_in, field_in, noise_in, lift_in, enc_recv_in, dec_send_in, dec_recv_in,
        mixing_in, expand_in, contract_in, readout_in, target_in, weight_in,
    )
    load = [pltpu.make_async_copy(o, i, loads.at[k]) for k, (o, i) in enumerate(zip(out_of, into))]
    for copy in load[:3]:
        copy.start()

    def peer_of(t):
        return ((z + far_first(t // NX, half)) % nz) * NX + (x + NX - 1 - t % NX) % NX

    barrier = pltpu.get_barrier_semaphore()

    def greet_band(t, carry):
        pl.semaphore_signal(barrier, inc=1, device_id={"band": peer_of(t)}, device_id_type=MESH)
        return carry

    def greet_member(k, carry):
        pl.semaphore_signal(
            barrier, inc=1, device_id={"member": (m + k) % members}, device_id_type=MESH
        )
        return carry

    lax.fori_loop(0, bands - 1, greet_band, 0)
    lax.fori_loop(1, members, greet_member, 0)
    for copy in load[3:]:
        copy.start()

    def to_slots(value, ref):
        ref[...] = value.reshape(ref.shape).astype(BF)

    def from_slots(ref):
        return ref[...].astype(F32).reshape(slots, PAD).astype(BF)

    def band_copy(src, dst, ssem, rsem, peer):
        return pltpu.make_async_remote_copy(
            src_ref=src, dst_ref=dst, send_sem=ssem, recv_sem=rsem,
            device_id={"band": peer}, device_id_type=MESH,
        )

    def member_copy(src, dst, ssem, rsem, peer):
        return pltpu.make_async_remote_copy(
            src_ref=src, dst_ref=dst, send_sem=ssem, recv_sem=rsem,
            device_id={"member": peer}, device_id_type=MESH,
        )

    def exchange(send, recv, ssem, rsem):
        def go(t, carry):
            peer = peer_of(t)
            band_copy(send.at[peer], recv.at[b], ssem, rsem, peer).start()
            return carry

        lax.fori_loop(0, bands - 1, go, 0)
        recv[pl.ds(b, 1)] = send[pl.ds(b, 1)]

    def whole(send, recv, ssem, rsem):
        some = pl.ds(0, bands - 1)
        return band_copy(send.at[some], recv.at[some], ssem, rsem, (b + 1) % bands)

    def fill_at(h):
        return fill[:, pl.ds(pl.multiple_of(h * cut, cut), cut)]

    for copy in load[:3]:
        copy.wait()
    inputs = pad_rows((field[...] + noise[...].astype(F32)).astype(BF).astype(F32), PAD).astype(BF)
    to_slots(dot(one_hot(enc_send, cells).astype(BF), inputs, 1, 1), send1)
    pl.semaphore_wait(barrier, bands - 1 + members - 1)
    exchange(send1, recv1, s1, r1)
    for copy in load[3:]:
        copy.wait()

    chips = members // 2
    partner = y * 2 + 1 - core
    for h in range(2):
        halves_b[h] = target[:, h * cut : (h + 1) * cut]
        weights[h] = weight[:, h * cut : (h + 1) * cut].astype(F32)

    def shared(src, dst, ssem, rsem):
        for k in (2, 1, 3):
            for c in range(2):
                to = ((y + k) % chips) * 2 + c
                member_copy(src.at[c], dst.at[m], ssem, rsem, to).start()
        member_copy(src.at[1 - core], dst.at[m], ssem, rsem, partner).start()
        dst[pl.ds(m, 1)] = src[pl.ds(core, 1)]

    shared(halves_b, teach, st, rt)

    land = one_hot(enc_recv, nodes).T
    enc_land[...] = land.astype(BF)
    edge_scale = 1.0 / jnp.maximum(jnp.sum(land, axis=1, keepdims=True), 1.0)
    lift_rows = pad_rows(lift[...].astype(F32), PAD).astype(BF)
    readp[...] = pad_rows(readout[...].astype(F32), PAD).astype(BF)
    both[...] = dot(contract[...], readp[...], 1, 1).astype(BF)
    pick = one_hot(dec_send, nodes)
    dec_pick[...] = pick.astype(BF)
    dec_land[...] = pick.T.astype(BF)
    cover = one_hot(dec_recv, cells)
    fill[...] = cover.astype(BF)
    inverse = 1.0 / jnp.maximum(jnp.sum(cover, axis=0, keepdims=True), 1.0)
    for h in range(2):
        inverses[h] = inverse[:, h * cut : (h + 1) * cut]

    whole(send1, recv1, s1, r1).wait_recv()
    embedded = dot(from_slots(recv1), lift_rows)
    rows = (embedded * sigmoid(embedded)).astype(BF)
    state[...] = dot(enc_land[...], rows) * edge_scale
    recip = lax.rsqrt(jnp.mean(state[...] * state[...], axis=1, keepdims=True) + norm_eps)
    normed = (state[...] * recip * mixing[...]).astype(BF)
    hidden_pre[...] = dot(normed, expand[...])
    gate = sigmoid(hidden_pre[...])
    hidden = (hidden_pre[...] * gate).astype(BF)
    next_b = (state[...] + dot(hidden, contract[...])).astype(BF)
    projected = dot(next_b, readp[...], 1, 1).astype(BF)
    to_slots(dot(dec_pick[...], projected), send2)
    exchange(send2, recv2, s2, r2)

    normed_t[...] = normed.astype(F32).T.astype(BF)
    hidden_t[...] = hidden.astype(F32).T.astype(BF)
    next_t[...] = next_b.astype(F32).T.astype(BF)
    dsilu[...] = gate * (1.0 + hidden_pre[...] * (1.0 - gate))

    seven = pl.ds(0, members - 1)
    every_target = member_copy(teach.at[seven], teach.at[seven], st, rt, (m + 1) % members)
    every_target.wait_recv()
    whole(send2, recv2, s2, r2).wait_recv()
    grid_sum = dot(from_slots(recv2), fill[...], 0, 0)[:channels]
    mine = field[...] + grid_sum * inverse
    stu[...] = mine

    for h in range(2):
        halves[h] = mine[:, h * cut : (h + 1) * cut]
    shared(halves, stus, ss, rs)
    stu[...] = mine
    every_student = member_copy(stus.at[seven], stus.at[seven], ss, rs, (m + 1) % members)
    every_student.wait_recv()
    both_mine = stus[pl.ds(y * 2, 2)]
    pull = jnp.zeros(both_mine.shape, F32)
    for j in range(members):
        pull = pull + (slope(both_mine - teach[j].astype(F32)) - slope(both_mine - stus[j]))
    pull = pull * (weights[pl.ds(core, 1)] * inverses[pl.ds(core, 1)])
    pieces[pl.ds(0, 2)] = pull.astype(BF)
    pass_on = member_copy(pieces.at[1 - core], pieces.at[2], sp, rp, partner)
    pass_on.start()
    first = pad_rows(pieces[pl.ds(core, 1)][0].astype(F32), PAD).astype(BF)
    picked = dot(fill_at(core), first, 1, 1)
    pass_on.wait_recv()
    second = pad_rows(pieces[2].astype(F32), PAD).astype(BF)
    to_slots(picked + dot(fill_at(1 - core), second, 1, 1), send3)
    exchange(send3, recv3, s3, r3)
    whole(send3, recv3, s3, r3).wait_recv()

    node_grad = dot(dec_land[...], from_slots(recv3)).astype(BF)
    blocks = sums[0].shape[:3]
    three = pl.ds(0, NX - 1)
    next_x = z * NX + (x + 1) % NX
    far_x = (2, 1, 3)

    pre = None
    for c, (kind, at, width) in enumerate(CHUNKS):
        if kind == "down":
            value = dot(hidden_t[...], node_grad)
        elif kind == "dec":
            value = dot(next_t[...], node_grad)
        else:
            if pre is None:
                pre = (dot(node_grad, both[...], 1, 1) * dsilu[...]).astype(BF)
            value = dot(normed_t[...], pre[:, at : at + width])
        sums[c][...] = value.reshape(*blocks, width).astype(BF)
        for k in far_x:
            to = (x + k) % NX
            band_copy(
                sums[c].at[to], from_x[c].at[k - 1], s_x.at[c], r_x.at[c], z * NX + to
            ).start()

    every_x = [
        band_copy(sums[c].at[three], from_x[c], s_x.at[c], r_x.at[c], next_x)
        for c in range(chunks)
    ]
    ring = pl.ds(0, nz - 1)
    next_z = ((z + 1) % nz) * NX + x
    for c in range(chunks):
        every_x[c].wait_recv()
        total = sums[c][pl.ds(x, 1)][0].astype(F32)
        for k in range(NX - 1):
            total = total + from_x[c][k].astype(F32)
        part[c][...] = total.astype(BF)

        def send_z(j, carry, c=c):
            to = (z + far_first(j, half)) % nz
            band_copy(
                part[c].at[to], from_z[c].at[z], s_z.at[c], r_z.at[c], to * NX + x
            ).start()
            return carry

        lax.fori_loop(0, nz - 1, send_z, 0)
        from_z[c][pl.ds(z, 1)] = part[c][pl.ds(z, 1)]

    next_grad = dot(node_grad, readp[...])
    gained = dot(pre, expand[...], 1, 1) * mixing[...]
    inner = jnp.mean(gained * state[...], axis=1, keepdims=True)
    grad_b[...] = (
        next_grad + recip * gained - state[...] * (recip * recip * recip) * inner
    ).astype(BF)

    every_z = [
        band_copy(from_z[c].at[ring], from_z[c].at[ring], s_z.at[c], r_z.at[c], next_z)
        for c in range(chunks)
    ]
    all_z = [
        band_copy(full[c].at[x, ring], full[c].at[x, ring], s_gz.at[c], r_gz.at[c], next_z)
        for c in range(chunks)
    ]
    all_x = [
        band_copy(full[c].at[three], full[c].at[three], s_gx.at[c], r_gx.at[c], next_x)
        for c in range(chunks)
    ]
    for c in range(chunks):
        every_z[c].wait_recv()
        piece = jnp.sum(from_z[c][...].astype(F32), axis=0).astype(BF)
        full[c][pl.ds(x, 1), pl.ds(z, 1)] = piece[None, None]

        def gather_z(j, carry, c=c):
            to = (z + far_first(j, half)) % nz
            mine_z = full[c].at[x, z]
            band_copy(mine_z, mine_z, s_gz.at[c], r_gz.at[c], to * NX + x).start()
            return carry

        lax.fori_loop(0, nz - 1, gather_z, 0)

    for c in range(chunks):
        all_z[c].wait_recv()
        mine_x = full[c].at[x]
        for k in far_x:
            band_copy(mine_x, mine_x, s_gx.at[c], r_gx.at[c], z * NX + (x + k) % NX).start()

    rows = blocks[0] * blocks[1] * blocks[2]
    gain = jnp.zeros((8, rows), F32)
    for c, (kind, at, width) in enumerate(CHUNKS):
        all_x[c].wait_recv()
        some = full[c][...].astype(F32).reshape(rows, width)
        if kind == "down":
            down_out[...] = dot(some.astype(BF), readp[...]) * factor
        elif kind == "dec":
            dec_out[...] = some.T[:channels] * factor
        else:
            some = some * factor
            up_out[:, at : at + width] = some
            terms = some * expand[:, at : at + width].astype(F32)
            main = terms.astype(BF)
            rest = (terms - main.astype(F32)).astype(BF)
            ones = jnp.ones((8, width), BF)
            gain = gain + dot(ones, main, 1, 1) + dot(ones, rest, 1, 1)
    gain_out[...] = gain[:1] / mixing[...]

    whole(send1, recv1, s1, r1).wait_send()
    whole(send2, recv2, s2, r2).wait_send()
    whole(send3, recv3, s3, r3).wait_send()
    every_target.wait_send()
    every_student.wait_send()
    pass_on.wait_send()
    for c in range(chunks):
        every_x[c].wait_send()
        every_z[c].wait_send()
        all_z[c].wait_send()
        all_x[c].wait_send()


def write_kernel(*refs):
    sems = refs[-1]
    count = len(refs) // 2
    copies = [pltpu.make_async_copy(refs[k], refs[count + k], sems.at[k]) for k in range(count)]
    for copy in copies:
        copy.start()
    for copy in copies:
        copy.wait()


def body(
    field, noise, target, weight, enc_send, enc_recv, dec_send, dec_recv,
    lift, mixing, expand, contract, readout,
):
    bands = lax.axis_size("band")
    members = lax.axis_size("member")
    nz = bands // NX
    channels, cells = field.shape
    nodes = cells
    cap = enc_send.shape[2]
    slots = bands * cap
    lat, hid = expand.shape
    chunks = len(CHUNKS)
    vmem = pl.BlockSpec(memory_space=pltpu.VMEM)
    hbm = pl.BlockSpec(memory_space=pltpu.HBM)
    cut = cells // 2
    block = (nz, lat // bands)

    def per_chunk(*lead):
        return [pltpu.VMEM((*lead, *block, width), BF) for _, _, width in CHUNKS]

    dma = pltpu.SemaphoreType.DMA
    mixing_row = mixing[None]
    read_t = readout.T
    slot_buffer = pltpu.VMEM((bands, cap, PAD), BF)
    ins = (
        enc_send[0].T, field, noise[0], lift, enc_recv[0].T, dec_send[0].T, dec_recv[0].T,
        mixing_row, expand, contract, read_t, target[0], weight,
    )
    factor = 1.0 / math.sqrt(bands * nodes)
    results = pl.pallas_call(
        functools.partial(step_kernel, factor),
        out_shape=(
            pltpu.VMEM((channels, cells), F32),
            pltpu.VMEM((nodes, lat), BF),
            pltpu.VMEM((lat, hid), F32),
            pltpu.VMEM((hid, lat), F32),
            pltpu.VMEM((channels, lat), F32),
            pltpu.VMEM((1, lat), F32),
        ),
        in_specs=[hbm] * len(ins),
        out_specs=(vmem,) * 6,
        scratch_shapes=[pltpu.VMEM(a.shape, a.dtype) for a in ins]
        + [slot_buffer] * 6
        + [
            pltpu.VMEM((members, channels, cut), BF),
            pltpu.VMEM((2, channels, cut), BF),
            pltpu.VMEM((2, channels, cut), F32),
            pltpu.VMEM((members, channels, cut), F32),
            pltpu.VMEM((2, channels, cut), F32),
            pltpu.VMEM((2, 1, cut), F32),
            pltpu.VMEM((3, channels, cut), BF),
            pltpu.VMEM((nodes, slots), BF),
            pltpu.VMEM((slots, nodes), BF),
            pltpu.VMEM((nodes, slots), BF),
            pltpu.VMEM((slots, cells), BF),
            pltpu.VMEM((PAD, lat), BF),
            pltpu.VMEM((hid, PAD), BF),
            pltpu.VMEM((lat, nodes), BF),
            pltpu.VMEM((hid, nodes), BF),
            pltpu.VMEM((lat, nodes), BF),
            pltpu.VMEM((nodes, lat), F32),
            pltpu.VMEM((nodes, hid), F32),
            pltpu.VMEM((nodes, hid), F32),
        ]
        + [dma((len(ins),))]
        + [dma(())] * 12
        + [dma((chunks,))] * 8
        + per_chunk(NX)
        + per_chunk(NX - 1)
        + per_chunk()
        + per_chunk()
        + per_chunk(NX),
        compiler_params=pltpu.CompilerParams(
            collective_id=0, has_side_effects=True, vmem_limit_bytes=40 << 20
        ),
        name="step",
    )(*(pltpu.with_memory_space_constraint(a, pltpu.HBM) for a in ins))
    student, grad, up, down, dec, gain = pl.pallas_call(
        write_kernel,
        out_shape=tuple(jax.ShapeDtypeStruct(a.shape, a.dtype) for a in results),
        in_specs=[vmem] * 6,
        out_specs=(hbm,) * 6,
        scratch_shapes=[dma((6,))],
        name="write",
    )(*(pltpu.with_memory_space_constraint(a, pltpu.VMEM) for a in results))
    return student[None], grad[None], up[None], down[None], dec.T[None], gain


def solution(mesh):
    return jax.shard_map(
        body,
        mesh=mesh,
        in_specs=(
            P(None, "band"),
            P("member", None, "band"),
            P("member", None, "band"),
            P(None, "band"),
            P("band", None, None),
            P("band", None, None),
            P("band", None, None),
            P("band", None, None),
            P(),
            P(),
            P(),
            P(),
            P(),
        ),
        out_specs=(
            P("member", None, "band"),
            P("member", "band", None),
            P("member", None, None),
            P("member", None, None),
            P("member", None, None),
            P("member", None),
        ),
        check_vma=False,
    )
```

```python
import functools
import math

import jax
import jax.numpy as jnp
from jax import lax
from jax.experimental import pallas as pl
from jax.experimental.pallas import tpu as pltpu
from jax.sharding import PartitionSpec as P

MESH = pl.DeviceIdType.MESH
BF = jnp.bfloat16
F32 = jnp.float32
NX = 4
PAD = 128
CHUNKS = (("down", 0, 128), ("dec", 0, 128), ("up", 0, 128), ("up", 128, 128), ("up", 256, 128), ("up", 384, 128))
smooth_sq = 0.01
norm_eps = 1e-05


def dot(a, b, ca=1, cb=0):
    return lax.dot_general(a, b, (((ca,), (cb,)), ((), ())), preferred_element_type=F32)


def slope(diff):
    return diff * lax.rsqrt(diff * diff + smooth_sq)


def sigmoid(v):
    return 0.5 + 0.5 * jnp.tanh(0.5 * v)


def pad_rows(a, rows):
    return jnp.concatenate([a, jnp.zeros((rows - a.shape[0], a.shape[1]), a.dtype)], axis=0)


def one_hot(table_ref, width):
    cap, bands = table_ref.shape
    slots = bands * cap
    table = table_ref[...].astype(F32).astype(BF)
    row = lax.broadcasted_iota(jnp.int32, (slots, bands), 0)
    col = lax.broadcasted_iota(jnp.int32, (slots, bands), 1)
    owner = jnp.where(row // cap == col, 1.0, 0.0).astype(BF)
    spread = dot(owner, table, 1, 1)
    row = lax.broadcasted_iota(jnp.int32, (slots, cap), 0)
    col = lax.broadcasted_iota(jnp.int32, (slots, cap), 1)
    spread = jnp.where(row % cap == col, spread, 0.0).astype(BF)
    wide = dot(spread, jnp.ones((cap, width), BF))
    lanes = lax.broadcasted_iota(jnp.int32, (slots, width), 1).astype(F32)
    return jnp.where(wide == lanes, 1.0, 0.0)


def far_first(j, half):
    return half + (1 - 2 * (j % 2)) * ((j + 1) // 2)


def step_kernel(
    factor, enc_send_in, field_in, noise_in, lift_in, enc_recv_in, dec_send_in, dec_recv_in,
    mixing_in, expand_in, contract_in, readout_in, target_in, weight_in,
    stu, grad_b, up_out, down_out, dec_out, gain_out,
    enc_send, field, noise, lift, enc_recv, dec_send, dec_recv,
    mixing, expand, contract, readout, target, weight,
    send1, recv1, send2, recv2, send3, recv3,
    teach, halves_b, halves, stus, weights, inverses, pulls, pieces, enc_land, dec_pick, dec_land, fill, readp, both,
    normed_t, hidden_t, next_t, state, hidden_pre, dsilu,
    loads, s1, r1, s2, r2, s3, r3, st, rt, pt, ss, rs, ps, sp, rp,
    s_x, r_x, s_z, r_z, s_gz, r_gz, s_gx, r_gx, *chunk_refs,
):
    bands = send1.shape[0]
    members = teach.shape[0]
    nz = bands // NX
    half = nz // 2
    chunks = len(CHUNKS)
    sums, from_x, part, from_z, full = (chunk_refs[k * chunks : (k + 1) * chunks] for k in range(5))
    b = lax.axis_index("band")
    m = lax.axis_index("member")
    z = b // NX
    x = b % NX
    y = m // 2
    core = m % 2
    slots = send1.shape[0] * send1.shape[1]
    channels, cells = field.shape
    nodes = cells
    cut = cells // 2

    into = (
        enc_send, field, noise, lift, enc_recv, dec_send, dec_recv,
        mixing, expand, contract, readout, target, weight,
    )
    out_of = (
        enc_send_in, field_in, noise_in, lift_in, enc_recv_in, dec_send_in, dec_recv_in,
        mixing_in, expand_in, contract_in, readout_in, target_in, weight_in,
    )
    load = [pltpu.make_async_copy(o, i, loads.at[k]) for k, (o, i) in enumerate(zip(out_of, into))]
    for copy in load[:3]:
        copy.start()

    def peer_of(t):
        k = t % NX
        step = (1 - k // 2) * (2 + k) + (k // 2) * (3 - k)
        return ((z + far_first(t // NX, half)) % nz) * NX + (x + step) % NX

    barrier = pltpu.get_barrier_semaphore()

    def greet_band(t, carry):
        pl.semaphore_signal(barrier, inc=1, device_id={"band": peer_of(t)}, device_id_type=MESH)
        return carry

    def greet_member(k, carry):
        pl.semaphore_signal(
            barrier, inc=1, device_id={"member": (m + k) % members}, device_id_type=MESH
        )
        return carry

    lax.fori_loop(0, bands - 1, greet_band, 0)
    lax.fori_loop(1, members, greet_member, 0)
    for copy in load[3:]:
        copy.start()

    def to_slots(value, ref):
        ref[...] = value.reshape(ref.shape).astype(BF)

    def from_slots(ref):
        return ref[...].astype(F32).reshape(slots, PAD).astype(BF)

    def band_copy(src, dst, ssem, rsem, peer):
        return pltpu.make_async_remote_copy(
            src_ref=src, dst_ref=dst, send_sem=ssem, recv_sem=rsem,
            device_id={"band": peer}, device_id_type=MESH,
        )

    def member_copy(src, dst, ssem, rsem, peer):
        return pltpu.make_async_remote_copy(
            src_ref=src, dst_ref=dst, send_sem=ssem, recv_sem=rsem,
            device_id={"member": peer}, device_id_type=MESH,
        )

    def exchange(send, recv, ssem, rsem):
        def go(t, carry):
            peer = peer_of(t)
            band_copy(send.at[peer], recv.at[b], ssem, rsem, peer).start()
            return carry

        lax.fori_loop(0, bands - 1, go, 0)
        recv[pl.ds(b, 1)] = send[pl.ds(b, 1)]

    def whole(send, recv, ssem, rsem):
        some = pl.ds(0, bands - 1)
        return band_copy(send.at[some], recv.at[some], ssem, rsem, (b + 1) % bands)

    def fill_at(h):
        return fill[:, pl.ds(pl.multiple_of(h * cut, cut), cut)]

    for copy in load[:3]:
        copy.wait()
    inputs = pad_rows((field[...] + noise[...].astype(F32)).astype(BF).astype(F32), PAD).astype(BF)
    to_slots(dot(one_hot(enc_send, cells).astype(BF), inputs, 1, 1), send1)
    pl.semaphore_wait(barrier, bands - 1 + members - 1)
    exchange(send1, recv1, s1, r1)
    for copy in load[3:]:
        copy.wait()

    chips = members // 2
    partner = y * 2 + 1 - core
    for h in range(2):
        halves_b[h] = target[:, h * cut : (h + 1) * cut]
        weights[h] = weight[:, h * cut : (h + 1) * cut].astype(F32)

    def shared(src, dst, ssem, rsem, psem):
        for k in (2, 1, 3):
            for c in range(2):
                to = ((y + k) % chips) * 2 + c
                member_copy(src.at[c], dst.at[m], ssem, rsem, to).start()
        near = member_copy(src.at[1 - core], dst.at[m], ssem, psem, partner)
        near.start()
        dst[pl.ds(m, 1)] = src[pl.ds(core, 1)]
        return near

    near_target = shared(halves_b, teach, st, rt, pt)

    land = one_hot(enc_recv, nodes).T
    enc_land[...] = land.astype(BF)
    edge_scale = 1.0 / jnp.maximum(jnp.sum(land, axis=1, keepdims=True), 1.0)
    lift_rows = pad_rows(lift[...].astype(F32), PAD).astype(BF)
    readp[...] = pad_rows(readout[...].astype(F32), PAD).astype(BF)
    both[...] = dot(contract[...], readp[...], 1, 1).astype(BF)
    pick = one_hot(dec_send, nodes)
    dec_pick[...] = pick.astype(BF)
    dec_land[...] = pick.T.astype(BF)
    cover = one_hot(dec_recv, cells)
    fill[...] = cover.astype(BF)
    inverse = 1.0 / jnp.maximum(jnp.sum(cover, axis=0, keepdims=True), 1.0)
    for h in range(2):
        inverses[h] = inverse[:, h * cut : (h + 1) * cut]

    whole(send1, recv1, s1, r1).wait_recv()
    embedded = dot(from_slots(recv1), lift_rows)
    rows = (embedded * sigmoid(embedded)).astype(BF)
    state[...] = dot(enc_land[...], rows) * edge_scale
    recip = lax.rsqrt(jnp.mean(state[...] * state[...], axis=1, keepdims=True) + norm_eps)
    normed = (state[...] * recip * mixing[...]).astype(BF)
    hidden_pre[...] = dot(normed, expand[...])
    gate = sigmoid(hidden_pre[...])
    hidden = (hidden_pre[...] * gate).astype(BF)
    next_b = (state[...] + dot(hidden, contract[...])).astype(BF)
    projected = dot(next_b, readp[...], 1, 1).astype(BF)
    to_slots(dot(dec_pick[...], projected), send2)
    exchange(send2, recv2, s2, r2)

    normed_t[...] = normed.astype(F32).T.astype(BF)
    hidden_t[...] = hidden.astype(F32).T.astype(BF)
    next_t[...] = next_b.astype(F32).T.astype(BF)
    dsilu[...] = gate * (1.0 + hidden_pre[...] * (1.0 - gate))

    seven = pl.ds(0, members - 1)
    six = pl.ds(0, members - 2)
    every_target = member_copy(teach.at[seven], teach.at[seven], st, rt, (m + 1) % members)
    member_copy(teach.at[six], teach.at[six], st, rt, (m + 1) % members).wait_recv()
    near_target.wait_recv()
    whole(send2, recv2, s2, r2).wait_recv()
    grid_sum = dot(from_slots(recv2), fill[...], 0, 0)[:channels]
    mine = field[...] + grid_sum * inverse
    stu[...] = mine

    for h in range(2):
        halves[h] = mine[:, h * cut : (h + 1) * cut]
    near_student = shared(halves, stus, ss, rs, ps)
    stu[...] = mine
    every_student = member_copy(stus.at[seven], stus.at[seven], ss, rs, (m + 1) % members)
    near_student.wait_recv()
    both_mine = stus[pl.ds(y * 2, 2)]
    pull = jnp.zeros(both_mine.shape, F32)
    for j in range(members):
        pull = pull + slope(both_mine - teach[j].astype(F32))
    pulls[...] = pull
    member_copy(stus.at[six], stus.at[six], ss, rs, (m + 1) % members).wait_recv()
    pull = pulls[...]
    for j in range(members):
        pull = pull - slope(both_mine - stus[j])
    pull = pull * (weights[pl.ds(core, 1)] * inverses[pl.ds(core, 1)])
    pieces[pl.ds(0, 2)] = pull.astype(BF)
    pass_on = member_copy(pieces.at[1 - core], pieces.at[2], sp, rp, partner)
    pass_on.start()
    first = pad_rows(pieces[pl.ds(core, 1)][0].astype(F32), PAD).astype(BF)
    picked = dot(fill_at(core), first, 1, 1)
    pass_on.wait_recv()
    second = pad_rows(pieces[2].astype(F32), PAD).astype(BF)
    to_slots(picked + dot(fill_at(1 - core), second, 1, 1), send3)
    exchange(send3, recv3, s3, r3)
    whole(send3, recv3, s3, r3).wait_recv()

    node_grad = dot(dec_land[...], from_slots(recv3)).astype(BF)
    blocks = sums[0].shape[:3]
    three = pl.ds(0, NX - 1)
    next_x = z * NX + (x + 1) % NX
    far_x = (2, 1, 3)

    pre = None
    for c, (kind, at, width) in enumerate(CHUNKS):
        if kind == "down":
            value = dot(hidden_t[...], node_grad)
        elif kind == "dec":
            value = dot(next_t[...], node_grad)
        else:
            if pre is None:
                pre = (dot(node_grad, both[...], 1, 1) * dsilu[...]).astype(BF)
            value = dot(normed_t[...], pre[:, at : at + width])
        sums[c][...] = value.reshape(*blocks, width).astype(BF)
        for k in far_x:
            to = (x + k) % NX
            band_copy(
                sums[c].at[to], from_x[c].at[k - 1], s_x.at[c], r_x.at[c], z * NX + to
            ).start()

    every_x = [
        band_copy(sums[c].at[three], from_x[c], s_x.at[c], r_x.at[c], next_x)
        for c in range(chunks)
    ]
    ring = pl.ds(0, nz - 1)
    next_z = ((z + 1) % nz) * NX + x
    for c in range(chunks):
        every_x[c].wait_recv()
        total = sums[c][pl.ds(x, 1)][0].astype(F32)
        for k in range(NX - 1):
            total = total + from_x[c][k].astype(F32)
        part[c][...] = total.astype(BF)

        def send_z(j, carry, c=c):
            to = (z + far_first(j, half)) % nz
            band_copy(
                part[c].at[to], from_z[c].at[z], s_z.at[c], r_z.at[c], to * NX + x
            ).start()
            return carry

        lax.fori_loop(0, nz - 1, send_z, 0)
        from_z[c][pl.ds(z, 1)] = part[c][pl.ds(z, 1)]

    next_grad = dot(node_grad, readp[...])
    gained = dot(pre, expand[...], 1, 1) * mixing[...]
    inner = jnp.mean(gained * state[...], axis=1, keepdims=True)
    grad_b[...] = (
        next_grad + recip * gained - state[...] * (recip * recip * recip) * inner
    ).astype(BF)

    every_z = [
        band_copy(from_z[c].at[ring], from_z[c].at[ring], s_z.at[c], r_z.at[c], next_z)
        for c in range(chunks)
    ]
    all_z = [
        band_copy(full[c].at[x, ring], full[c].at[x, ring], s_gz.at[c], r_gz.at[c], next_z)
        for c in range(chunks)
    ]
    all_x = [
        band_copy(full[c].at[three], full[c].at[three], s_gx.at[c], r_gx.at[c], next_x)
        for c in range(chunks)
    ]
    for c in range(chunks):
        every_z[c].wait_recv()
        piece = jnp.sum(from_z[c][...].astype(F32), axis=0).astype(BF)
        full[c][pl.ds(x, 1), pl.ds(z, 1)] = piece[None, None]

        def gather_z(j, carry, c=c):
            to = (z + far_first(j, half)) % nz
            mine_z = full[c].at[x, z]
            band_copy(mine_z, mine_z, s_gz.at[c], r_gz.at[c], to * NX + x).start()
            return carry

        lax.fori_loop(0, nz - 1, gather_z, 0)

    for c in range(chunks):
        all_z[c].wait_recv()
        mine_x = full[c].at[x]
        for k in far_x:
            band_copy(mine_x, mine_x, s_gx.at[c], r_gx.at[c], z * NX + (x + k) % NX).start()

    rows = blocks[0] * blocks[1] * blocks[2]
    gain = jnp.zeros((8, rows), F32)
    for c, (kind, at, width) in enumerate(CHUNKS):
        all_x[c].wait_recv()
        some = full[c][...].astype(F32).reshape(rows, width)
        if kind == "down":
            down_out[...] = dot(some.astype(BF), readp[...]) * factor
        elif kind == "dec":
            dec_out[...] = some.T[:channels] * factor
        else:
            some = some * factor
            up_out[:, at : at + width] = some
            terms = some * expand[:, at : at + width].astype(F32)
            main = terms.astype(BF)
            rest = (terms - main.astype(F32)).astype(BF)
            ones = jnp.ones((8, width), BF)
            gain = gain + dot(ones, main, 1, 1) + dot(ones, rest, 1, 1)
    gain_out[...] = gain[:1] / mixing[...]

    whole(send1, recv1, s1, r1).wait_send()
    whole(send2, recv2, s2, r2).wait_send()
    whole(send3, recv3, s3, r3).wait_send()
    every_target.wait_send()
    every_student.wait_send()
    pass_on.wait_send()
    for c in range(chunks):
        every_x[c].wait_send()
        every_z[c].wait_send()
        all_z[c].wait_send()
        all_x[c].wait_send()


def write_kernel(*refs):
    sems = refs[-1]
    count = len(refs) // 2
    copies = [pltpu.make_async_copy(refs[k], refs[count + k], sems.at[k]) for k in range(count)]
    for copy in copies:
        copy.start()
    for copy in copies:
        copy.wait()


def body(
    field, noise, target, weight, enc_send, enc_recv, dec_send, dec_recv,
    lift, mixing, expand, contract, readout,
):
    bands = lax.axis_size("band")
    members = lax.axis_size("member")
    nz = bands // NX
    channels, cells = field.shape
    nodes = cells
    cap = enc_send.shape[2]
    slots = bands * cap
    lat, hid = expand.shape
    chunks = len(CHUNKS)
    vmem = pl.BlockSpec(memory_space=pltpu.VMEM)
    hbm = pl.BlockSpec(memory_space=pltpu.HBM)
    cut = cells // 2
    block = (nz, lat // bands)

    def per_chunk(*lead):
        return [pltpu.VMEM((*lead, *block, width), BF) for _, _, width in CHUNKS]

    dma = pltpu.SemaphoreType.DMA
    mixing_row = mixing[None]
    read_t = readout.T
    slot_buffer = pltpu.VMEM((bands, cap, PAD), BF)
    ins = (
        enc_send[0].T, field, noise[0], lift, enc_recv[0].T, dec_send[0].T, dec_recv[0].T,
        mixing_row, expand, contract, read_t, target[0], weight,
    )
    factor = 1.0 / math.sqrt(bands * nodes)
    results = pl.pallas_call(
        functools.partial(step_kernel, factor),
        out_shape=(
            pltpu.VMEM((channels, cells), F32),
            pltpu.VMEM((nodes, lat), BF),
            pltpu.VMEM((lat, hid), F32),
            pltpu.VMEM((hid, lat), F32),
            pltpu.VMEM((channels, lat), F32),
            pltpu.VMEM((1, lat), F32),
        ),
        in_specs=[hbm] * len(ins),
        out_specs=(vmem,) * 6,
        scratch_shapes=[pltpu.VMEM(a.shape, a.dtype) for a in ins]
        + [slot_buffer] * 6
        + [
            pltpu.VMEM((members, channels, cut), BF),
            pltpu.VMEM((2, channels, cut), BF),
            pltpu.VMEM((2, channels, cut), F32),
            pltpu.VMEM((members, channels, cut), F32),
            pltpu.VMEM((2, channels, cut), F32),
            pltpu.VMEM((2, 1, cut), F32),
            pltpu.VMEM((2, channels, cut), F32),
            pltpu.VMEM((3, channels, cut), BF),
            pltpu.VMEM((nodes, slots), BF),
            pltpu.VMEM((slots, nodes), BF),
            pltpu.VMEM((nodes, slots), BF),
            pltpu.VMEM((slots, cells), BF),
            pltpu.VMEM((PAD, lat), BF),
            pltpu.VMEM((hid, PAD), BF),
            pltpu.VMEM((lat, nodes), BF),
            pltpu.VMEM((hid, nodes), BF),
            pltpu.VMEM((lat, nodes), BF),
            pltpu.VMEM((nodes, lat), F32),
            pltpu.VMEM((nodes, hid), F32),
            pltpu.VMEM((nodes, hid), F32),
        ]
        + [dma((len(ins),))]
        + [dma(())] * 14
        + [dma((chunks,))] * 8
        + per_chunk(NX)
        + per_chunk(NX - 1)
        + per_chunk()
        + per_chunk()
        + per_chunk(NX),
        compiler_params=pltpu.CompilerParams(
            collective_id=0, has_side_effects=True, vmem_limit_bytes=40 << 20
        ),
        name="step",
    )(*(pltpu.with_memory_space_constraint(a, pltpu.HBM) for a in ins))
    student, grad, up, down, dec, gain = pl.pallas_call(
        write_kernel,
        out_shape=tuple(jax.ShapeDtypeStruct(a.shape, a.dtype) for a in results),
        in_specs=[vmem] * 6,
        out_specs=(hbm,) * 6,
        scratch_shapes=[dma((6,))],
        name="write",
    )(*(pltpu.with_memory_space_constraint(a, pltpu.VMEM) for a in results))
    return student[None], grad[None], up[None], down[None], dec.T[None], gain


def solution(mesh):
    return jax.shard_map(
        body,
        mesh=mesh,
        in_specs=(
            P(None, "band"),
            P("member", None, "band"),
            P("member", None, "band"),
            P(None, "band"),
            P("band", None, None),
            P("band", None, None),
            P("band", None, None),
            P("band", None, None),
            P(),
            P(),
            P(),
            P(),
            P(),
        ),
        out_specs=(
            P("member", None, "band"),
            P("member", "band", None),
            P("member", None, None),
            P("member", None, None),
            P("member", None, None),
            P("member", None),
        ),
        check_vma=False,
    )
```

```python
import functools
import math

import jax
import jax.numpy as jnp
from jax import lax
from jax.experimental import pallas as pl
from jax.experimental.pallas import tpu as pltpu
from jax.sharding import PartitionSpec as P

MESH = pl.DeviceIdType.MESH
BF = jnp.bfloat16
F32 = jnp.float32
NX = 4
PAD = 128
CHUNKS = (("down", 0, 128), ("dec", 0, 128), ("up", 0, 128), ("up", 128, 128), ("up", 256, 128), ("up", 384, 128))
smooth_sq = 0.01
norm_eps = 1e-05


def dot(a, b, ca=1, cb=0):
    return lax.dot_general(a, b, (((ca,), (cb,)), ((), ())), preferred_element_type=F32)


def slope(diff):
    return diff * lax.rsqrt(diff * diff + smooth_sq)


def sigmoid(v):
    return 0.5 + 0.5 * jnp.tanh(0.5 * v)


def pad_rows(a, rows):
    return jnp.concatenate([a, jnp.zeros((rows - a.shape[0], a.shape[1]), a.dtype)], axis=0)


def one_hot(table_ref, width):
    cap, bands = table_ref.shape
    slots = bands * cap
    table = table_ref[...].astype(F32).astype(BF)
    row = lax.broadcasted_iota(jnp.int32, (slots, bands), 0)
    col = lax.broadcasted_iota(jnp.int32, (slots, bands), 1)
    owner = jnp.where(row // cap == col, 1.0, 0.0).astype(BF)
    spread = dot(owner, table, 1, 1)
    row = lax.broadcasted_iota(jnp.int32, (slots, cap), 0)
    col = lax.broadcasted_iota(jnp.int32, (slots, cap), 1)
    spread = jnp.where(row % cap == col, spread, 0.0).astype(BF)
    wide = dot(spread, jnp.ones((cap, width), BF))
    lanes = lax.broadcasted_iota(jnp.int32, (slots, width), 1).astype(F32)
    return jnp.where(wide == lanes, 1.0, 0.0)


def far_first(j, half):
    return half + (1 - 2 * (j % 2)) * ((j + 1) // 2)


def step_kernel(
    factor, enc_send_in, field_in, noise_in, lift_in, enc_recv_in, dec_send_in, dec_recv_in,
    mixing_in, expand_in, contract_in, readout_in, target_in, weight_in,
    stu, grad_b, up_out, down_out, dec_out, gain_out,
    enc_send, field, noise, lift, enc_recv, dec_send, dec_recv,
    mixing, expand, contract, readout, target, weight,
    send1, recv1, send2, recv2, send3, recv3,
    teach, halves_b, halves, stus, weights, inverses, pulls, pieces, enc_land, dec_pick, dec_land, fill, readp, both,
    normed_t, hidden_t, next_t, state, hidden_pre, dsilu,
    loads, s1, r1, s2, r2, s3, r3, st, rt, pt, ss, rs, ps, sp, rp,
    s_x, r_x, s_z, r_z, s_gz, r_gz, s_gx, r_gx, *chunk_refs,
):
    bands = send1.shape[0]
    members = teach.shape[0]
    nz = bands // NX
    half = nz // 2
    chunks = len(CHUNKS)
    sums, from_x, part, from_z, full = (chunk_refs[k * chunks : (k + 1) * chunks] for k in range(5))
    b = lax.axis_index("band")
    m = lax.axis_index("member")
    z = b // NX
    x = b % NX
    y = m // 2
    core = m % 2
    slots = send1.shape[0] * send1.shape[1]
    channels, cells = field.shape
    nodes = cells
    cut = cells // 2

    into = (
        enc_send, field, noise, lift, enc_recv, dec_send, dec_recv,
        mixing, expand, contract, readout, target, weight,
    )
    out_of = (
        enc_send_in, field_in, noise_in, lift_in, enc_recv_in, dec_send_in, dec_recv_in,
        mixing_in, expand_in, contract_in, readout_in, target_in, weight_in,
    )
    load = [pltpu.make_async_copy(o, i, loads.at[k]) for k, (o, i) in enumerate(zip(out_of, into))]
    for copy in load[:3]:
        copy.start()

    def peer_of(t):
        k = t % NX
        step = (1 - k // 2) * (2 + k) + (k // 2) * (3 - k)
        return ((z + far_first(t // NX, half)) % nz) * NX + (x + step) % NX

    barrier = pltpu.get_barrier_semaphore()

    def greet_band(t, carry):
        pl.semaphore_signal(barrier, inc=1, device_id={"band": peer_of(t)}, device_id_type=MESH)
        return carry

    def greet_member(k, carry):
        pl.semaphore_signal(
            barrier, inc=1, device_id={"member": (m + k) % members}, device_id_type=MESH
        )
        return carry

    lax.fori_loop(0, bands - 1, greet_band, 0)
    lax.fori_loop(1, members, greet_member, 0)
    for copy in load[3:]:
        copy.start()

    def to_slots(value, ref):
        ref[...] = value.reshape(ref.shape).astype(BF)

    def from_slots(ref):
        return ref[...].astype(F32).reshape(slots, PAD).astype(BF)

    def band_copy(src, dst, ssem, rsem, peer):
        return pltpu.make_async_remote_copy(
            src_ref=src, dst_ref=dst, send_sem=ssem, recv_sem=rsem,
            device_id={"band": peer}, device_id_type=MESH,
        )

    def member_copy(src, dst, ssem, rsem, peer):
        return pltpu.make_async_remote_copy(
            src_ref=src, dst_ref=dst, send_sem=ssem, recv_sem=rsem,
            device_id={"member": peer}, device_id_type=MESH,
        )

    def exchange(send, recv, ssem, rsem):
        def go(t, carry):
            peer = peer_of(t)
            band_copy(send.at[peer], recv.at[b], ssem, rsem, peer).start()
            return carry

        lax.fori_loop(0, bands - 1, go, 0)
        recv[pl.ds(b, 1)] = send[pl.ds(b, 1)]

    def whole(send, recv, ssem, rsem):
        some = pl.ds(0, bands - 1)
        return band_copy(send.at[some], recv.at[some], ssem, rsem, (b + 1) % bands)

    def fill_at(h):
        return fill[:, pl.ds(pl.multiple_of(h * cut, cut), cut)]

    for copy in load[:3]:
        copy.wait()
    inputs = pad_rows((field[...] + noise[...].astype(F32)).astype(BF).astype(F32), PAD).astype(BF)
    to_slots(dot(one_hot(enc_send, cells).astype(BF), inputs, 1, 1), send1)
    pl.semaphore_wait(barrier, bands - 1 + members - 1)
    exchange(send1, recv1, s1, r1)
    for copy in load[3:]:
        copy.wait()

    chips = members // 2
    partner = y * 2 + 1 - core
    for h in range(2):
        halves_b[h] = target[:, h * cut : (h + 1) * cut]
        weights[h] = weight[:, h * cut : (h + 1) * cut].astype(F32)

    def shared(src, dst, ssem, rsem, psem):
        for k in (2, 1, 3):
            for c in range(2):
                to = ((y + k) % chips) * 2 + c
                member_copy(src.at[c], dst.at[m], ssem, rsem, to).start()
        near = member_copy(src.at[1 - core], dst.at[m], ssem, psem, partner)
        near.start()
        dst[pl.ds(m, 1)] = src[pl.ds(core, 1)]
        return near

    near_target = shared(halves_b, teach, st, rt, pt)

    land = one_hot(enc_recv, nodes).T
    enc_land[...] = land.astype(BF)
    edge_scale = 1.0 / jnp.maximum(jnp.sum(land, axis=1, keepdims=True), 1.0)
    lift_rows = pad_rows(lift[...].astype(F32), PAD).astype(BF)
    readp[...] = pad_rows(readout[...].astype(F32), PAD).astype(BF)
    both[...] = dot(contract[...], readp[...], 1, 1).astype(BF)
    pick = one_hot(dec_send, nodes)
    dec_pick[...] = pick.astype(BF)
    dec_land[...] = pick.T.astype(BF)
    cover = one_hot(dec_recv, cells)
    fill[...] = cover.astype(BF)
    inverse = 1.0 / jnp.maximum(jnp.sum(cover, axis=0, keepdims=True), 1.0)
    for h in range(2):
        inverses[h] = inverse[:, h * cut : (h + 1) * cut]

    whole(send1, recv1, s1, r1).wait_recv()
    embedded = dot(from_slots(recv1), lift_rows)
    rows = (embedded * sigmoid(embedded)).astype(BF)
    state[...] = dot(enc_land[...], rows) * edge_scale
    recip = lax.rsqrt(jnp.mean(state[...] * state[...], axis=1, keepdims=True) + norm_eps)
    normed = (state[...] * recip * mixing[...]).astype(BF)
    hidden_pre[...] = dot(normed, expand[...])
    gate = sigmoid(hidden_pre[...])
    hidden = (hidden_pre[...] * gate).astype(BF)
    next_b = (state[...] + dot(hidden, contract[...])).astype(BF)
    projected = dot(next_b, readp[...], 1, 1).astype(BF)
    to_slots(dot(dec_pick[...], projected), send2)
    exchange(send2, recv2, s2, r2)

    normed_t[...] = normed.astype(F32).T.astype(BF)
    hidden_t[...] = hidden.astype(F32).T.astype(BF)
    next_t[...] = next_b.astype(F32).T.astype(BF)
    dsilu[...] = gate * (1.0 + hidden_pre[...] * (1.0 - gate))

    seven = pl.ds(0, members - 1)
    six = pl.ds(0, members - 2)
    every_target = member_copy(teach.at[seven], teach.at[seven], st, rt, (m + 1) % members)
    member_copy(teach.at[six], teach.at[six], st, rt, (m + 1) % members).wait_recv()
    near_target.wait_recv()
    whole(send2, recv2, s2, r2).wait_recv()
    grid_sum = dot(from_slots(recv2), fill[...], 0, 0)[:channels]
    mine = field[...] + grid_sum * inverse
    stu[...] = mine

    for h in range(2):
        halves[h] = mine[:, h * cut : (h + 1) * cut]
    near_student = shared(halves, stus, ss, rs, ps)
    stu[...] = mine
    every_student = member_copy(stus.at[seven], stus.at[seven], ss, rs, (m + 1) % members)
    near_student.wait_recv()
    both_mine = stus[pl.ds(y * 2, 2)]
    pull = jnp.zeros(both_mine.shape, F32)
    for j in range(members):
        pull = pull + slope(both_mine - teach[j].astype(F32))
    pulls[...] = pull
    member_copy(stus.at[six], stus.at[six], ss, rs, (m + 1) % members).wait_recv()
    pull = pulls[...]
    for j in range(members):
        pull = pull - slope(both_mine - stus[j])
    pull = pull * (weights[pl.ds(core, 1)] * inverses[pl.ds(core, 1)])
    pieces[pl.ds(0, 2)] = pull.astype(BF)
    pass_on = member_copy(pieces.at[1 - core], pieces.at[2], sp, rp, partner)
    pass_on.start()
    first = pad_rows(pieces[pl.ds(core, 1)][0].astype(F32), PAD).astype(BF)
    picked = dot(fill_at(core), first, 1, 1)
    pass_on.wait_recv()
    second = pad_rows(pieces[2].astype(F32), PAD).astype(BF)
    to_slots(picked + dot(fill_at(1 - core), second, 1, 1), send3)
    exchange(send3, recv3, s3, r3)
    whole(send3, recv3, s3, r3).wait_recv()

    node_grad = dot(dec_land[...], from_slots(recv3)).astype(BF)
    blocks = sums[0].shape[:3]
    three = pl.ds(0, NX - 1)
    next_x = z * NX + (x + 1) % NX
    far_x = (2, 1, 3)

    pre = None
    for c, (kind, at, width) in enumerate(CHUNKS):
        if kind == "down":
            value = dot(hidden_t[...], node_grad)
        elif kind == "dec":
            value = dot(next_t[...], node_grad)
        else:
            if pre is None:
                pre = (dot(node_grad, both[...], 1, 1) * dsilu[...]).astype(BF)
            if at % (2 * width) == 0:
                two = dot(normed_t[...], pre[:, at : at + 2 * width])
            first = at % (2 * width)
            value = two[:, first : first + width]
        sums[c][...] = value.reshape(*blocks, width).astype(BF)
        for k in far_x:
            to = (x + k) % NX
            band_copy(
                sums[c].at[to], from_x[c].at[k - 1], s_x.at[c], r_x.at[c], z * NX + to
            ).start()

    every_x = [
        band_copy(sums[c].at[three], from_x[c], s_x.at[c], r_x.at[c], next_x)
        for c in range(chunks)
    ]
    ring = pl.ds(0, nz - 1)
    next_z = ((z + 1) % nz) * NX + x
    for c in range(chunks):
        every_x[c].wait_recv()
        total = sums[c][pl.ds(x, 1)][0].astype(F32)
        for k in range(NX - 1):
            total = total + from_x[c][k].astype(F32)
        part[c][...] = total.astype(BF)

        def send_z(j, carry, c=c):
            to = (z + far_first(j, half)) % nz
            band_copy(
                part[c].at[to], from_z[c].at[z], s_z.at[c], r_z.at[c], to * NX + x
            ).start()
            return carry

        lax.fori_loop(0, nz - 1, send_z, 0)
        from_z[c][pl.ds(z, 1)] = part[c][pl.ds(z, 1)]

    next_grad = dot(node_grad, readp[...])
    gained = dot(pre, expand[...], 1, 1) * mixing[...]
    inner = jnp.mean(gained * state[...], axis=1, keepdims=True)
    grad_b[...] = (
        next_grad + recip * gained - state[...] * (recip * recip * recip) * inner
    ).astype(BF)

    every_z = [
        band_copy(from_z[c].at[ring], from_z[c].at[ring], s_z.at[c], r_z.at[c], next_z)
        for c in range(chunks)
    ]
    all_z = [
        band_copy(full[c].at[x, ring], full[c].at[x, ring], s_gz.at[c], r_gz.at[c], next_z)
        for c in range(chunks)
    ]
    all_x = [
        band_copy(full[c].at[three], full[c].at[three], s_gx.at[c], r_gx.at[c], next_x)
        for c in range(chunks)
    ]
    for c in range(chunks):
        every_z[c].wait_recv()
        piece = jnp.sum(from_z[c][...].astype(F32), axis=0).astype(BF)
        full[c][pl.ds(x, 1), pl.ds(z, 1)] = piece[None, None]

        def gather_z(j, carry, c=c):
            to = (z + far_first(j, half)) % nz
            mine_z = full[c].at[x, z]
            band_copy(mine_z, mine_z, s_gz.at[c], r_gz.at[c], to * NX + x).start()
            return carry

        lax.fori_loop(0, nz - 1, gather_z, 0)

    for c in range(chunks):
        all_z[c].wait_recv()
        mine_x = full[c].at[x]
        for k in far_x:
            band_copy(mine_x, mine_x, s_gx.at[c], r_gx.at[c], z * NX + (x + k) % NX).start()

    rows = blocks[0] * blocks[1] * blocks[2]
    gain = jnp.zeros((8, rows), F32)
    for c, (kind, at, width) in enumerate(CHUNKS):
        all_x[c].wait_recv()
        some = full[c][...].astype(F32).reshape(rows, width)
        if kind == "down":
            down_out[...] = dot(some.astype(BF), readp[...]) * factor
        elif kind == "dec":
            dec_out[...] = some.T[:channels] * factor
        else:
            some = some * factor
            up_out[:, at : at + width] = some
            terms = some * expand[:, at : at + width].astype(F32)
            main = terms.astype(BF)
            rest = (terms - main.astype(F32)).astype(BF)
            ones = jnp.ones((8, 2 * width), BF)
            gain = gain + dot(ones, jnp.concatenate([main, rest], axis=1), 1, 1)
    gain_out[...] = gain[:1] / mixing[...]

    whole(send1, recv1, s1, r1).wait_send()
    whole(send2, recv2, s2, r2).wait_send()
    whole(send3, recv3, s3, r3).wait_send()
    every_target.wait_send()
    every_student.wait_send()
    pass_on.wait_send()
    for c in range(chunks):
        every_x[c].wait_send()
        every_z[c].wait_send()
        all_z[c].wait_send()
        all_x[c].wait_send()


def write_kernel(*refs):
    sems = refs[-1]
    count = len(refs) // 2
    copies = [pltpu.make_async_copy(refs[k], refs[count + k], sems.at[k]) for k in range(count)]
    for k in sorted(range(count), key=lambda k: -math.prod(refs[k].shape)):
        copies[k].start()
    for copy in copies:
        copy.wait()


def body(
    field, noise, target, weight, enc_send, enc_recv, dec_send, dec_recv,
    lift, mixing, expand, contract, readout,
):
    bands = lax.axis_size("band")
    members = lax.axis_size("member")
    nz = bands // NX
    channels, cells = field.shape
    nodes = cells
    cap = enc_send.shape[2]
    slots = bands * cap
    lat, hid = expand.shape
    chunks = len(CHUNKS)
    vmem = pl.BlockSpec(memory_space=pltpu.VMEM)
    hbm = pl.BlockSpec(memory_space=pltpu.HBM)
    cut = cells // 2
    block = (nz, lat // bands)

    def per_chunk(*lead):
        return [pltpu.VMEM((*lead, *block, width), BF) for _, _, width in CHUNKS]

    dma = pltpu.SemaphoreType.DMA
    mixing_row = mixing[None]
    read_t = readout.T
    slot_buffer = pltpu.VMEM((bands, cap, PAD), BF)
    ins = (
        enc_send[0].T, field, noise[0], lift, enc_recv[0].T, dec_send[0].T, dec_recv[0].T,
        mixing_row, expand, contract, read_t, target[0], weight,
    )
    factor = 1.0 / math.sqrt(bands * nodes)
    results = pl.pallas_call(
        functools.partial(step_kernel, factor),
        out_shape=(
            pltpu.VMEM((channels, cells), F32),
            pltpu.VMEM((nodes, lat), BF),
            pltpu.VMEM((lat, hid), F32),
            pltpu.VMEM((hid, lat), F32),
            pltpu.VMEM((channels, lat), F32),
            pltpu.VMEM((1, lat), F32),
        ),
        in_specs=[hbm] * len(ins),
        out_specs=(vmem,) * 6,
        scratch_shapes=[pltpu.VMEM(a.shape, a.dtype) for a in ins]
        + [slot_buffer] * 6
        + [
            pltpu.VMEM((members, channels, cut), BF),
            pltpu.VMEM((2, channels, cut), BF),
            pltpu.VMEM((2, channels, cut), F32),
            pltpu.VMEM((members, channels, cut), F32),
            pltpu.VMEM((2, channels, cut), F32),
            pltpu.VMEM((2, 1, cut), F32),
            pltpu.VMEM((2, channels, cut), F32),
            pltpu.VMEM((3, channels, cut), BF),
            pltpu.VMEM((nodes, slots), BF),
            pltpu.VMEM((slots, nodes), BF),
            pltpu.VMEM((nodes, slots), BF),
            pltpu.VMEM((slots, cells), BF),
            pltpu.VMEM((PAD, lat), BF),
            pltpu.VMEM((hid, PAD), BF),
            pltpu.VMEM((lat, nodes), BF),
            pltpu.VMEM((hid, nodes), BF),
            pltpu.VMEM((lat, nodes), BF),
            pltpu.VMEM((nodes, lat), F32),
            pltpu.VMEM((nodes, hid), F32),
            pltpu.VMEM((nodes, hid), F32),
        ]
        + [dma((len(ins),))]
        + [dma(())] * 14
        + [dma((chunks,))] * 8
        + per_chunk(NX)
        + per_chunk(NX - 1)
        + per_chunk()
        + per_chunk()
        + per_chunk(NX),
        compiler_params=pltpu.CompilerParams(
            collective_id=0, has_side_effects=True, vmem_limit_bytes=40 << 20
        ),
        name="step",
    )(*(pltpu.with_memory_space_constraint(a, pltpu.HBM) for a in ins))
    student, grad, up, down, dec, gain = pl.pallas_call(
        write_kernel,
        out_shape=tuple(jax.ShapeDtypeStruct(a.shape, a.dtype) for a in results),
        in_specs=[vmem] * 6,
        out_specs=(hbm,) * 6,
        scratch_shapes=[dma((6,))],
        name="write",
    )(*(pltpu.with_memory_space_constraint(a, pltpu.VMEM) for a in results))
    return student[None], grad[None], up[None], down[None], dec.T[None], gain


def solution(mesh):
    return jax.shard_map(
        body,
        mesh=mesh,
        in_specs=(
            P(None, "band"),
            P("member", None, "band"),
            P("member", None, "band"),
            P(None, "band"),
            P("band", None, None),
            P("band", None, None),
            P("band", None, None),
            P("band", None, None),
            P(),
            P(),
            P(),
            P(),
            P(),
        ),
        out_specs=(
            P("member", None, "band"),
            P("member", "band", None),
            P("member", None, None),
            P("member", None, None),
            P("member", None, None),
            P("member", None),
        ),
        check_vma=False,
    )
```
